512 devices in a mesh: gx: 8 (over z_hi, x), gy: 8 (over y, core), gz: 8 (over z_lo).
Axes of the slice: x: 4, y: 4, z: 16 (z_hi: 2, z_lo: 8; z = z_hi * 8 + z_lo), core: 2. Of those that a mesh axis runs over, the one named last changes fastest.
Arguments:
- grains: float32 [12, 64, 128, 1024], P(None, 'gz', 'gx', 'gy'), may hold values from 0 to 0.6
- solute: float32 [64, 128, 1024], P('gz', 'gx', 'gy'), may hold values from 0 to 0.6
- thermal: float32 [8, 8, 8, 40, 4096], P('gz', 'gx', 'gy'), may hold values from 0.5 to 1.5
- block_slot: int32 [8, 8, 8, 20], P('gz', 'gx', 'gy'), may hold values from -1 to 39, as said below
- block_owner: int32 [8, 8, 8, 20], P('gz', 'gx', 'gy'), may hold values from -1 to 7, as said below
- block_offset: int32 [8, 8, 8, 3, 20], P('gz', 'gx', 'gy'), may hold values from -31 to 128, as said below
Outputs:
- grains_out: float32 [12, 64, 128, 1024], P(None, 'gz', 'gx', 'gy')
- solute_out: float32 [64, 128, 1024], P('gz', 'gx', 'gy')
- temperature: float32 [64, 128, 1024], P('gz', 'gx', 'gy')
The draws below stay inside these ranges and needn't reach their ends.
Inputs may be any that keep to these rules, and one draw needn't show every extreme that they name: `block_slot`: -1 exactly where block_owner is -1; the live entries of all tiles name distinct pairs (owner, slot) within a column. `block_owner`: -1 marks an empty entry. No owner serves more than 5 live entries of one tile; in every draw, in each column, some owner serves 5 entries of every tile of that column; and in every draw some tile of the box has all 20 entries live. `block_offset`: 0 for empty entries. Along each dimension the live starts of a tile differ by multiples of 32, and the hats of a tile's live blocks sum to one at each of its cells.
All inputs are finite; a program needn't handle non-finite values.
Results may differ from the reference program's by a relative error of at most 0.0003.
Values sent between devices are 32-bit elements; how exact they have to be, the bound alone decides.
A program may use at most 64 MiB of HBM per device.

```python
import jax
import jax.numpy as jnp
from jax import lax

GRAINS = 12
BLOCK = 16
STEPS = 3
CZ = 8
CX = 16
CY = 128
SPAN = 32
KZ = 2
KX = 2
KY = 5
MAXB = 20
CAP = 5
TILES_Z = 8
TILES_X = 8
TILES_Y = 8
SLOTS = 40
NZ = 64
NX = 128
NY = 1024


def axis_blocks(phases, length, reach_count):
    steps_index = jnp.arange(reach_count, dtype=jnp.int32)
    usable = steps_index[None, None, None, :] <= (length + phases[..., None]) // SPAN
    anchor = SPAN * steps_index[None, None, None, :] - phases[..., None]
    return (usable, anchor)


def layout(key):
    folded = jax.random.fold_in(key, 4242)
    subkeys = jax.random.split(folded, 5)
    tile_grid = (TILES_Z, TILES_X, TILES_Y)
    tiles = TILES_Z * TILES_X * TILES_Y
    phases = jax.random.randint(subkeys[0], tile_grid + (3,), 0, SPAN)
    chosen = jax.random.randint(subkeys[1], (), 0, tiles)
    numbered = jnp.arange(tiles, dtype=jnp.int32).reshape(tile_grid)
    phases = jnp.where((numbered == chosen)[..., None], SPAN - 1, phases)
    usable_z, anchor_z = axis_blocks(phases[..., 0], CZ, KZ)
    usable_x, anchor_x = axis_blocks(phases[..., 1], CX, KX)
    usable_y, anchor_y = axis_blocks(phases[..., 2], CY, KY)
    full_shape = tile_grid + (KZ, KX, KY)
    usable = usable_z[..., :, None, None] & usable_x[..., None, :, None] & usable_y[..., None, None, :]
    usable = usable.reshape(tile_grid + (MAXB,))
    corner_z = jnp.broadcast_to(anchor_z[..., :, None, None], full_shape).reshape(tile_grid + (MAXB,))
    corner_x = jnp.broadcast_to(anchor_x[..., None, :, None], full_shape).reshape(tile_grid + (MAXB,))
    corner_y = jnp.broadcast_to(anchor_y[..., None, None, :], full_shape).reshape(tile_grid + (MAXB,))
    corners = jnp.stack([corner_z, corner_x, corner_y], axis=3)
    scores = jax.random.randint(subkeys[2], tile_grid + (MAXB,), 0, 1 << 20) * MAXB + jnp.arange(MAXB, dtype=jnp.int32)
    shuffle = jnp.argsort(scores, axis=-1)
    usable = jnp.take_along_axis(usable, shuffle, axis=-1)
    corners = jnp.take_along_axis(corners, jnp.broadcast_to(shuffle[..., None, :], corners.shape), axis=-1)
    counted = jnp.maximum(jnp.cumsum(usable.astype(jnp.int32), axis=-1) - 1, 0)
    ranked = jax.random.randint(subkeys[3], (TILES_X, TILES_Y, TILES_Z), 0, 1 << 20) * TILES_Z + jnp.arange(TILES_Z, dtype=jnp.int32)
    column_order = jnp.argsort(ranked, axis=-1).astype(jnp.int32)
    holder_rank = counted // CAP
    z_index = jnp.arange(TILES_Z, dtype=jnp.int32)[:, None, None, None]
    x_index = jnp.arange(TILES_X, dtype=jnp.int32)[None, :, None, None]
    y_index = jnp.arange(TILES_Y, dtype=jnp.int32)[None, None, :, None]
    holders = column_order[x_index, y_index, holder_rank]
    placed = jax.random.randint(subkeys[4], (TILES_Z, TILES_X, TILES_Y, SLOTS), 0, 1 << 20) * SLOTS + jnp.arange(SLOTS, dtype=jnp.int32)
    slot_order = jnp.argsort(placed, axis=-1).astype(jnp.int32)
    seat_index = z_index * CAP + counted % CAP
    slot_ids = slot_order[holders, x_index, y_index, seat_index]
    holders = jnp.where(usable, holders, -1).astype(jnp.int32)
    slot_ids = jnp.where(usable, slot_ids, -1).astype(jnp.int32)
    corners = jnp.where(usable[..., None, :], corners, 0).astype(jnp.int32)
    return (slot_ids, holders, corners)


def draw_block_slot(key, part):
    return layout(key)[0]


def draw_block_owner(key, part):
    return layout(key)[1]


def draw_block_offset(key, part):
    return layout(key)[2]


def levels(key, shape, cuts, smallest, high):
    gain = 1.0
    for position, parts in cuts:
        draws = jax.random.uniform(jax.random.fold_in(jax.random.fold_in(key, 6), position), (parts,), jnp.float32, smallest / len(cuts), high / len(cuts))
        gain = gain * jnp.repeat(jnp.exp(draws), shape[position] // parts).reshape((-1,) + (1,) * (len(shape) - 1 - position))
    return gain


def setup_inputs(seed: int = 0) -> dict:
    arg_keys = jax.random.split(jax.random.key(seed), 7)
    grains = jnp.clip(0.6 * jax.random.uniform(arg_keys[0], (GRAINS, NZ, NX, NY), jnp.float32) ** levels(arg_keys[0], (GRAINS, NZ, NX, NY), ((1, 8), (2, 8), (3, 8)), -0.2, 0.2), 0.0, 0.6)
    solute = jnp.clip(0.6 * jax.random.uniform(arg_keys[1], (NZ, NX, NY), jnp.float32) ** levels(arg_keys[1], (NZ, NX, NY), ((0, 8), (1, 8), (2, 8)), -0.2, 0.2), 0.0, 0.6)
    thermal = jnp.clip(0.5 + 1.0 * jax.random.uniform(arg_keys[2], (TILES_Z, TILES_X, TILES_Y, SLOTS, BLOCK ** 3), jnp.float32) ** levels(arg_keys[2], (TILES_Z, TILES_X, TILES_Y, SLOTS, BLOCK ** 3), ((0, 8), (1, 8), (2, 8)), -0.2, 0.2), 0.5, 1.5)
    block_slot = draw_block_slot(jax.random.fold_in(arg_keys[6], 71), 0)
    block_owner = draw_block_owner(jax.random.fold_in(arg_keys[6], 71), 0)
    block_offset = draw_block_offset(jax.random.fold_in(arg_keys[6], 71), 0)
    return dict(grains=grains, solute=solute, thermal=thermal, block_slot=block_slot, block_owner=block_owner, block_offset=block_offset)


step_rate = 0.1
stiffness = 1.6
cross_energy = 0.25
drive_scale = 2.0
liquidus_slope = 0.5
rejection = 0.5
diffusion_rate = 0.15


def hat_weights(starts, cell_count):
    positions = jnp.arange(cell_count, dtype=jnp.float32)
    node_sites = 2.0 * jnp.arange(BLOCK, dtype=jnp.float32)
    distance = positions[None, :, None] - starts.astype(jnp.float32)[:, None, None] - node_sites[None, None, :]
    return jnp.maximum(0.0, 1.0 - jnp.abs(distance) / 2.0)


def project(blocks, starts, live_entry, layers, breadth, length):
    entries = blocks.shape[0]
    cubes = blocks.reshape(entries, BLOCK, BLOCK, BLOCK)
    weight_z = hat_weights(starts[0], layers) * live_entry.astype(jnp.float32)[:, None, None]
    weight_x = hat_weights(starts[1], breadth)
    weight_y = hat_weights(starts[2], length)
    along_y = jnp.einsum("epqr,eyr->epqy", cubes, weight_y, precision=lax.Precision.HIGHEST)
    along_x = jnp.einsum("exq,epqy->epxy", weight_x, along_y, precision=lax.Precision.HIGHEST)
    return weight_z, along_x


def laplace(padded):
    middle = padded[..., 1:-1, 1:-1, 1:-1]
    return (padded[..., 2:, 1:-1, 1:-1] + padded[..., :-2, 1:-1, 1:-1]
            + padded[..., 1:-1, 2:, 1:-1] + padded[..., 1:-1, :-2, 1:-1]
            + padded[..., 1:-1, 1:-1, 2:] + padded[..., 1:-1, 1:-1, :-2] - 6.0 * middle)


def advance(padded, heat_field):
    orders = padded[:-1]
    concentration = padded[-1]
    squares = jnp.sum(orders * orders, axis=0)
    bending = laplace(orders)
    diffusion_term = laplace(concentration - rejection * squares)
    central = orders[:, 1:-1, 1:-1, 1:-1]
    central_sum = squares[1:-1, 1:-1, 1:-1]
    central_solute = concentration[1:-1, 1:-1, 1:-1]
    undercool = drive_scale * (1.0 - heat_field - liquidus_slope * central_solute)
    double_well = 2.0 * central * (1.0 - central) * (1.0 - 2.0 * central)
    contact_term = 4.0 * cross_energy * central * (central_sum - central * central)
    growth_term = 30.0 * central * central * (1.0 - central) * (1.0 - central) * undercool
    new_orders = central + step_rate * (stiffness * bending - double_well - contact_term + growth_term)
    new_solute = central_solute + diffusion_rate * diffusion_term
    return jnp.concatenate([new_orders, new_solute[None]], axis=0)


def tile_heat(flat_tile, thermal, block_slot, block_owner, block_offset):
    tile_layer = flat_tile // (TILES_X * TILES_Y)
    tile_row = (flat_tile // TILES_Y) % TILES_X
    tile_col = flat_tile % TILES_Y
    slot_ids = block_slot[tile_layer, tile_row, tile_col]
    holders = block_owner[tile_layer, tile_row, tile_col]
    starts = block_offset[tile_layer, tile_row, tile_col]
    live_entry = holders >= 0
    blocks = thermal[jnp.clip(holders, 0, TILES_Z - 1), tile_row, tile_col, jnp.clip(slot_ids, 0, SLOTS - 1)]
    weight_z, along_x = project(blocks, starts, live_entry, CZ, CX, CY)
    return jnp.einsum("ezp,epxy->zxy", weight_z, along_x, precision=lax.Precision.HIGHEST)


def reference(grains, solute, thermal, block_slot, block_owner, block_offset):
    tiles = jnp.arange(TILES_Z * TILES_X * TILES_Y, dtype=jnp.int32)
    pieces = lax.map(lambda flat_tile: tile_heat(flat_tile, thermal, block_slot, block_owner, block_offset), tiles)
    pieces = pieces.reshape(TILES_Z, TILES_X, TILES_Y, CZ, CX, CY)
    heat_field = jnp.transpose(pieces, (0, 3, 1, 4, 2, 5)).reshape(NZ, NX, NY)
    fields = jnp.concatenate([grains, solute[None]], axis=0)
    for repeat in range(STEPS):
        padded = jnp.pad(fields, ((0, 0), (0, 0), (1, 1), (1, 1)), mode="wrap")
        padded = jnp.pad(padded, ((0, 0), (1, 1), (0, 0), (0, 0)), mode="symmetric")
        fields = advance(padded, heat_field)
    return fields[:-1], fields[-1], heat_field
```

```python
import jax
import jax.numpy as jnp
from jax import lax
from jax.experimental import pallas as pl
from jax.experimental.pallas import tpu as pltpu
from jax.sharding import PartitionSpec as P

F32 = jnp.float32
BF16 = jnp.bfloat16
MESH = pl.DeviceIdType.MESH
NF = 14
SOL = 12
HEAT = 13
KEY, HZ, HX, HY, LIVE, TILE = range(6)
AX = 9
NODES = 48
LOW, HIGH = 14, 15


def iota(shape, axis):
    return lax.broadcasted_iota(jnp.int32, shape, axis)


def split(x):
    high = x.astype(BF16)
    return high, (x - high.astype(F32)).astype(BF16)


def nt(a, b):
    return lax.dot_general(a, b, (((1,), (1,)), ((), ())), preferred_element_type=F32)


def main_neighbours(below, row, above, low, high, r):
    lane = iota(row.shape, 1)
    left = jnp.where(lane == 0, pltpu.roll(low, (128 - (r * 8 + 3)) % 128, 1), pltpu.roll(row, 1, 1))
    right = jnp.where(lane == 127, pltpu.roll(high, (127 - (r * 8 + 4)) % 128, 1), pltpu.roll(row, 127, 1))
    return (below + above) + (pltpu.roll(row, 1, 0) + pltpu.roll(row, 23, 0)) + (left + right)


def strip_neighbours(v):
    return (
        (pltpu.roll(v, 8, 1) + pltpu.roll(v, 120, 1))
        + (pltpu.roll(v, 1, 1) + pltpu.roll(v, 127, 1))
        + (pltpu.roll(v, 1, 0) + pltpu.roll(v, 23, 0))
    )


def grown(c, around, s, drive):
    cc = c * c
    w = c - cc
    rate = w * ((4.0 * c - 2.0) + w * drive) + c * (cc - s)
    return 0.04 * c + 0.16 * around + 0.1 * rate


def kernel(
    tiles,
    grains, solute, thermal, slots, owners, offsets,
    grains_out, solute_out, heat_out,
    ext, alt, bend, squares, drives,
    xp, xr, dp, dr, pk, yr,
    req, rq, lb, prm, xs, gr, gx,
    s_rq, r_rq, s_gx, r_gx, s_z, r_z, s_x, r_x, s_zt, r_zt, s_xt, r_xt, s_d, r_d, s_y, r_y,
):
    me = lax.axis_index("gz")
    ix, iy = lax.axis_index("gx"), lax.axis_index("gy")
    nx, ny = lax.axis_size("gx"), lax.axis_size("gy")
    xside = ({"gx": lax.rem(ix + nx - 1, nx)}, {"gx": lax.rem(ix + 1, nx)})
    yside = ({"gy": lax.rem(iy + ny - 1, ny)}, {"gy": lax.rem(iy + 1, ny)})
    others = [{"gz": lax.rem(me + k, tiles)} for k in range(1, tiles)]
    has_low, has_high = me > 0, me < tiles - 1
    zside = ({"gz": jnp.maximum(me - 1, 0)}, {"gz": jnp.minimum(me + 1, tiles - 1)})
    has = (has_low, has_high)

    barrier = pltpu.get_barrier_semaphore()
    partners = [*xside, *yside, *others]
    for d in partners:
        pl.semaphore_signal(barrier, inc=1, device_id=d, device_id_type=MESH)

    def remote(src, dst, ss, rs, d):
        return pltpu.make_async_remote_copy(
            src_ref=src, dst_ref=dst, send_sem=ss, recv_sem=rs, device_id=d, device_id_type=MESH
        )

    live = owners[...] >= 0
    livef = live.astype(F32)
    off = offsets[...]
    half = (off + (off & 1)) >> 1
    req[...] = jnp.zeros((8, 128), F32)
    req[KEY : KEY + 1, 0:20] = jnp.where(live, owners[...] * 64 + slots[...], -1).astype(F32)
    req[HZ : HZ + 3, 0:20] = half.astype(F32) * livef
    req[LIVE : LIVE + 1, 0:20] = livef
    req[TILE : TILE + 1, 0:20] = livef * me.astype(F32)

    for s, first in ((0, 0), (1, 13)):
        def pack(f, _, s=s, first=first):
            for i in range(3):
                xp[s, f, i * 8 : i * 8 + 8, :] = grains[f, :, first + i, :]
            return 0
        lax.fori_loop(0, 12, pack, 0)
        for i in range(3):
            xp[s, SOL, i * 8 : i * 8 + 8, :] = solute[:, first + i, :]

    pl.semaphore_wait(barrier, len(partners))

    request = [
        remote(req, rq.at[me], s_rq.at[k], r_rq.at[me], d) for k, d in enumerate(others)
    ]
    for c in request:
        c.start()
    xcopy = [
        remote(xp.at[0, 0:13], xr.at[1, 0:13], s_x.at[0], r_x.at[1], xside[0]),
        remote(xp.at[1, 0:13], xr.at[0, 0:13], s_x.at[1], r_x.at[0], xside[1]),
    ]
    for c in xcopy:
        c.start()
    zrows = ((0, 11), (5, 0))
    zcopy = []
    for d in range(2):
        a, b = zrows[d]
        zcopy.append((
            remote(grains.at[:, a : a + 3], ext.at[0:12, b : b + 3, 0:16], s_z.at[d], r_z.at[d], zside[d]),
            remote(solute.at[a : a + 3], ext.at[SOL, b : b + 3, 0:16], s_z.at[2 + d], r_z.at[2 + d], zside[d]),
        ))

        @pl.when(has[d])
        def _(d=d):
            for c in zcopy[d]:
                c.start()

    def place(f, _):
        for z in range(8):
            ext[f, 3 + z, 0:16, :] = grains[f, z]
        return 0
    lax.fori_loop(0, 12, place, 0)
    for z in range(8):
        ext[SOL, 3 + z, 0:16, :] = solute[z]

    row8, lane8 = iota((8, 128), 0), iota((8, 128), 1) >> 4
    def turn(g, _):
        rows = pl.ds(pl.multiple_of(g * 8, 8), 8)
        for c in range(32):
            v = thermal[rows, c * 128 : c * 128 + 128]
            for k in (1, 2, 4):
                rb, lbit = (row8 & k) != 0, (lane8 & k) != 0
                a = pltpu.roll(pltpu.roll(v, 8 - k, 0), 16 * k, 1)
                b = pltpu.roll(pltpu.roll(v, k, 0), 128 - 16 * k, 1)
                v = jnp.where(rb == lbit, v, jnp.where(lbit, a, b))
            lb[g, c // 2, (c % 2) * 8 : (c % 2) * 8 + 8, :] = v
        return 0
    lax.fori_loop(0, 5, turn, 0)
    rq[me] = req[...]
    xs[...] = jnp.zeros(xs.shape, F32)

    for k in range(1, tiles):
        src = lax.rem(me + tiles - k, tiles)
        remote(req, rq.at[src], s_rq.at[k - 1], r_rq.at[src], others[k - 1]).wait_recv()

    lists = [jnp.zeros((8, 128), F32), jnp.zeros((8, 128), F32)]
    for t in range(tiles):
        v = rq[t]
        lists[t // 4] = lists[t // 4] + (pltpu.roll(v, 32 * (t % 4), 1) if t % 4 else v)
    for h in range(2):
        prm[5 + h] = lists[h]
    base = me * 64
    for g in range(5):
        slot_of = base + g * 8 + (iota((128, 128), 0) >> 4)
        total = jnp.zeros((8, 128), F32)
        for h in range(2):
            match = jnp.where(lists[h][KEY : KEY + 1, :] == slot_of.astype(F32), 1.0, 0.0).astype(BF16)
            total = total + nt(lists[h].astype(BF16), match)
        prm[g] = total

    def choose(g, _):
        v = prm[g]
        hz, hx = v[HZ : HZ + 1, :], v[HX : HX + 1, :]
        layers = [jnp.zeros((16, 128), F32) for _ in range(5)]
        for p in range(16):
            part = lb[g, p]
            for a in range(5):
                layers[a] = layers[a] + jnp.where(hz == float(a - p), part, 0.0)
        at = iota((16, 128), 0).astype(F32) + hx
        lanes = pl.ds(pl.multiple_of(g * 128, 128), 128)
        for a in range(5):
            for b in range(AX):
                xs[a * AX + b : a * AX + b + 1, lanes] = jnp.sum(
                    jnp.where(at == float(b), layers[a], 0.0), axis=0, keepdims=True
                )
        return 0
    lax.fori_loop(0, 5, choose, 0)

    hi, lo = split(xs[...])
    both = jnp.concatenate([hi, lo], axis=0)
    where_to = []
    for g in range(5):
        v = prm[g]
        spot = v[HY : HY + 1, :] + 128.0 * v[TILE : TILE + 1, :] + (iota((1, 128), 1) & 15).astype(F32)
        where_to.append(jnp.where(v[LIVE : LIVE + 1, :] > 0.5, spot, -4096.0))
    where_to = jnp.concatenate(where_to, axis=1)
    answer = []
    for k in range(tiles - 1, -1, -1):
        t = lax.rem(me + k, tiles)
        line = (iota((128, 640), 0) + t * 128).astype(F32)
        onto = jnp.where(line == where_to, 1.0, 0.0).astype(BF16)
        out = nt(both, onto)
        gr[t] = out[0:NODES] + out[NODES : 2 * NODES]
        if k:
            c = remote(gr.at[t], gx.at[me], s_gx.at[k - 1], r_gx.at[me], others[k - 1])
            c.start()
            answer.append(c)

    def unpack_x(f):
        for z in range(8):
            ext[f, 3 + z, 16:19, :] = xr[1, f, pl.ds(z, 3, stride=8), :]
            ext[f, 3 + z, 21:24, :] = xr[0, f, pl.ds(z, 3, stride=8), :]

    parity = jnp.max(jnp.where(live, off & 1, 0).astype(F32), axis=1, keepdims=True)
    bz, bx, by = parity[0:1], parity[1:2], parity[2:3]
    node, cell = iota((128, 128), 0), iota((128, 128), 1).astype(F32)
    wy = jnp.maximum(0.0, 1.0 - jnp.abs(cell - (2.0 * node.astype(F32) - by)) * 0.5)
    wy = jnp.where(node <= 64, wy, 0.0).astype(BF16)
    ci, ki = iota((128, NODES), 0), iota((128, NODES), 1)
    az = (ki * 57) >> 9
    ax = ki - AX * az
    wz = jnp.maximum(0.0, 1.0 - jnp.abs((ci >> 4).astype(F32) - (2.0 * az.astype(F32) - bz)) * 0.5)
    wx = jnp.maximum(0.0, 1.0 - jnp.abs((ci & 15).astype(F32) - (2.0 * ax.astype(F32) - bx)) * 0.5)
    wzx = (wz * wx).astype(BF16)

    grid = gr[me]
    for k in range(1, tiles):
        src = lax.rem(me + tiles - k, tiles)
        remote(gr.at[src], gx.at[src], s_gx.at[k - 1], r_gx.at[src], others[k - 1]).wait_recv()
        grid = grid + gx[src]
    hi, lo = split(grid)
    fine = jnp.dot(jnp.concatenate([hi, lo], axis=0), wy, preferred_element_type=F32)
    fine = fine[0:NODES] + fine[NODES : 2 * NODES]
    hi, lo = split(fine)
    heat = jnp.dot(wzx, hi, preferred_element_type=F32) + jnp.dot(wzx, lo, preferred_element_type=F32)
    heat = heat.reshape(8, 16, 128)
    heat_out[...] = heat
    for z in range(8):
        ext[HEAT, 3 + z, 0:16, :] = heat[z]
    for s, first in ((0, 0), (1, 13)):
        for i in range(3):
            xp[s, HEAT, i * 8 : i * 8 + 8, :] = heat[:, first + i, :]
    xheat = [
        remote(xp.at[0, HEAT], xr.at[1, HEAT], s_xt.at[0], r_xt.at[1], xside[0]),
        remote(xp.at[1, HEAT], xr.at[0, HEAT], s_xt.at[1], r_xt.at[0], xside[1]),
    ]
    for c in xheat:
        c.start()
    zheat = []
    for d in range(2):
        a, b = zrows[d]
        zheat.append(remote(
            ext.at[HEAT, 3 + a : 6 + a, 0:16], ext.at[HEAT, b : b + 3, 0:16], s_zt.at[d], r_zt.at[d], zside[d]
        ))

        @pl.when(has[d])
        def _(d=d):
            zheat[d].start()

    for c in xcopy:
        c.wait_recv()
    for c in xheat:
        c.wait_recv()

    order = ((2, 1), (0, 1))
    shown = ((0, 1), (7, 6))
    dcopy = []
    for d in range(2):
        for s in range(2):
            near, far = order[s]
            z1, z2 = shown[d]
            for k, (i, z) in enumerate(((near, z1), (near, z2), (far, z1))):
                for f in range(NF):
                    dp[2 * d + s, k, f : f + 1, :] = xr[s, f, i * 8 + z : i * 8 + z + 1, :]
            dcopy.append(remote(
                dp.at[2 * d + s], dr.at[2 * d + s], s_d.at[2 * d + s], r_d.at[2 * d + s], zside[d]
            ))

        @pl.when(has[d])
        def _(d=d):
            for s in range(2):
                dcopy[2 * d + s].start()

    def unpack_all(f, _):
        unpack_x(f)
        return 0
    lax.fori_loop(0, NF, unpack_all, 0)

    for d in range(2):
        @pl.when(has[1 - d])
        def _(d=d):
            for c in zcopy[d]:
                c.wait_recv()
            zheat[d].wait_recv()
            for s in range(2):
                dcopy[2 * d + s].wait_recv()
            e1, e2 = ((11, 12), (2, 1))[d]
            for s in range(2):
                x1, x2 = ((23, 22), (16, 17))[s]
                for k, (e, x) in enumerate(((e1, x1), (e2, x1), (e1, x2))):
                    for f in range(NF):
                        ext[f, e, x : x + 1, :] = dr[2 * d + s, k, f : f + 1, :]

        @pl.when(jnp.logical_not(has[1 - d]))
        def _(d=d):
            def mirror(f, _):
                for i in range(3):
                    if d:
                        ext[f, 2 - i] = ext[f, 3 + i]
                    else:
                        ext[f, 11 + i] = ext[f, 10 - i]
                return 0
            lax.fori_loop(0, NF, mirror, 0)

    slot = iota((24, 128), 1) >> 3
    def pack_y(f, _):
        v = jnp.zeros((24, 128), F32)
        for r in range(14):
            v = jnp.where(slot == r, pltpu.roll(ext[f, r], r * 8 + 4, 1), v)
        pk[f] = v
        return 0
    lax.fori_loop(0, NF, pack_y, 0)
    ycopy = [
        remote(pk, yr.at[1], s_y.at[0], r_y.at[1], yside[0]),
        remote(pk, yr.at[0], s_y.at[1], r_y.at[0], yside[1]),
    ]
    for c in ycopy:
        c.start()
    for c in ycopy:
        c.wait_recv()
    upper = (iota((24, 128), 1) & 7) >= 4
    def unpack_y(f, _):
        own = pk[f]
        ext[f, LOW] = jnp.where(upper, own, yr[0, f])
        ext[f, HIGH] = jnp.where(upper, yr[1, f], own)
        return 0
    lax.fori_loop(0, NF, unpack_y, 0)

    def step(src, dst, first, last):
        def sums(r, _):
            s = src[0, r] * src[0, r]
            for f in range(1, 12):
                s = s + src[f, r] * src[f, r]
            u = src[SOL, r]
            squares[r] = s
            bend[r] = u - 0.5 * s
            drives[r] = 60.0 * (1.0 - ext[HEAT, r] - 0.5 * u)
            return 0
        lax.fori_loop(0, 16, sums, 0)
        final = dst is None

        def fields(f, _):
            low, high = src[f, LOW], src[f, HIGH]
            for r in range(first, last):
                c = src[f, r]
                around = main_neighbours(src[f, r - 1], c, src[f, r + 1], low, high, r)
                v = grown(c, around, squares[r], drives[r])
                if final:
                    grains_out[f, r - 3] = v[0:16]
                else:
                    dst[f, r] = v
            if not final:
                for r, c in ((LOW, low), (HIGH, high)):
                    dst[f, r] = grown(c, strip_neighbours(c), squares[r], drives[r])
            return 0
        lax.fori_loop(0, 12, fields, 0)
        low, high = bend[LOW], bend[HIGH]
        for r in range(first, last):
            c = bend[r]
            lap = main_neighbours(bend[r - 1], c, bend[r + 1], low, high, r) - 6.0 * c
            v = src[SOL, r] + 0.15 * lap
            if final:
                solute_out[r - 3] = v[0:16]
            else:
                dst[SOL, r] = v
        if not final:
            for r, c in ((LOW, low), (HIGH, high)):
                dst[SOL, r] = src[SOL, r] + 0.15 * (strip_neighbours(c) - 6.0 * c)

    step(ext, alt, 1, 13)
    step(alt, ext, 2, 12)
    step(ext, None, 3, 11)

    for c in [*request, *xcopy, *answer, *xheat, *ycopy]:
        c.wait_send()
    for d in range(2):
        @pl.when(has[d])
        def _(d=d):
            for c in (*zcopy[d], zheat[d], dcopy[2 * d], dcopy[2 * d + 1]):
                c.wait_send()


def body(grains, solute, thermal, block_slot, block_owner, block_offset):
    tiles = lax.axis_size("gz")
    vmem = pl.BlockSpec(memory_space=pltpu.VMEM)
    dma = pltpu.SemaphoreType.DMA
    import functools

    return pl.pallas_call(
        functools.partial(kernel, tiles),
        out_shape=(
            jax.ShapeDtypeStruct(grains.shape, F32),
            jax.ShapeDtypeStruct(solute.shape, F32),
            jax.ShapeDtypeStruct(solute.shape, F32),
        ),
        in_specs=[vmem] * 6,
        out_specs=(vmem,) * 3,
        scratch_shapes=[
            pltpu.VMEM((NF, 16, 24, 128), F32),
            pltpu.VMEM((13, 16, 24, 128), F32),
            pltpu.VMEM((16, 24, 128), F32),
            pltpu.VMEM((16, 24, 128), F32),
            pltpu.VMEM((16, 24, 128), F32),
            pltpu.VMEM((2, NF, 24, 128), F32),
            pltpu.VMEM((2, NF, 24, 128), F32),
            pltpu.VMEM((4, 3, 16, 128), F32),
            pltpu.VMEM((4, 3, 16, 128), F32),
            pltpu.VMEM((NF, 24, 128), F32),
            pltpu.VMEM((2, NF, 24, 128), F32),
            pltpu.VMEM((8, 128), F32),
            pltpu.VMEM((tiles, 8, 128), F32),
            pltpu.VMEM((5, 16, 16, 128), F32),
            pltpu.VMEM((7, 8, 128), F32),
            pltpu.VMEM((NODES, 640), F32),
            pltpu.VMEM((tiles, NODES, 128), F32),
            pltpu.VMEM((tiles, NODES, 128), F32),
            dma((tiles,)), dma((tiles,)), dma((tiles,)), dma((tiles,)),
            dma((4,)), dma((4,)), dma((2,)), dma((2,)),
            dma((2,)), dma((2,)), dma((2,)), dma((2,)),
            dma((4,)), dma((4,)), dma((2,)), dma((2,)),
        ],
        compiler_params=pltpu.CompilerParams(
            collective_id=0, has_side_effects=True, vmem_limit_bytes=48 * 1024 * 1024
        ),
    )(
        grains,
        solute,
        thermal.reshape(thermal.shape[3], thermal.shape[4]),
        block_slot.reshape(1, -1),
        block_owner.reshape(1, -1),
        block_offset.reshape(3, -1),
    )


def solution(mesh):
    in_specs = (
        P(None, "gz", "gx", "gy"),
        P("gz", "gx", "gy"),
        P("gz", "gx", "gy", None, None),
        P("gz", "gx", "gy", None),
        P("gz", "gx", "gy", None),
        P("gz", "gx", "gy", None, None),
    )
    out_specs = (P(None, "gz", "gx", "gy"), P("gz", "gx", "gy"), P("gz", "gx", "gy"))
    return jax.shard_map(body, mesh=mesh, in_specs=in_specs, out_specs=out_specs, check_vma=False)
```

```python
import jax
import jax.numpy as jnp
from jax import lax
from jax.experimental import pallas as pl
from jax.experimental.pallas import tpu as pltpu
from jax.sharding import PartitionSpec as P

F32 = jnp.float32
BF16 = jnp.bfloat16
MESH = pl.DeviceIdType.MESH
NF = 14
SOL = 12
HEAT = 13
DIRECT = 7
KEY, HZ, HX, HY, LIVE, TILE = range(6)
AX = 9
NODES = 48
LOW, HIGH = 14, 15


def iota(shape, axis):
    return lax.broadcasted_iota(jnp.int32, shape, axis)


def split(x):
    high = x.astype(BF16)
    return high, (x - high.astype(F32)).astype(BF16)


def nt(a, b):
    return lax.dot_general(a, b, (((1,), (1,)), ((), ())), preferred_element_type=F32)


def edges(low, high):
    return jnp.where((iota(low.shape, 1) & 7) == 3, low, pltpu.roll(high, 126, 1))


def main_neighbours(below, row, above, edge, r):
    n = below.shape[0]
    lane = iota(below.shape, 1)
    beyond = pltpu.roll(edge, (125 - r * 8) % 128, 1)
    inside = row[0:n]
    left = jnp.where(lane == 0, beyond, pltpu.roll(inside, 1, 1))
    right = jnp.where(lane == 127, beyond, pltpu.roll(inside, 127, 1))
    return (below + above) + (pltpu.roll(row, 1, 0)[0:n] + pltpu.roll(row, 23, 0)[0:n]) + (left + right)


def strip_neighbours(v):
    return (
        (pltpu.roll(v, 8, 1) + pltpu.roll(v, 120, 1))
        + (pltpu.roll(v, 1, 1) + pltpu.roll(v, 127, 1))
        + (pltpu.roll(v, 1, 0) + pltpu.roll(v, 23, 0))
    )


def grown(c, around, s, drive):
    cc = c * c
    w = c - cc
    rate = w * ((4.0 * c - 2.0) + w * drive) + c * (cc - s)
    return 0.04 * c + 0.16 * around + 0.1 * rate


def kernel(
    tiles,
    grains, solute, thermal, slots, owners, offsets,
    grains_out, solute_out, heat_out,
    ext, alt, bend, squares, drives,
    xp, xr, relay, dp, dr, pk, yr,
    hk, hy, hxz, hxy, hyz,
    stored, lists_in, req, rq, lb, prm, xs, gr, gx,
    loads, s_rq, r_rq, s_gx, r_gx, s_z, r_z, s_x, r_x, s_zt, r_zt, s_xt, r_xt, s_d, r_d, s_y, r_y,
    s_relay, r_relay, s_hy, r_hy, s_hxz, r_hxz, s_hxy, r_hxy, s_hyz, r_hyz,
):
    me = lax.axis_index("gz")
    ix, iy = lax.axis_index("gx"), lax.axis_index("gy")
    nx, ny = lax.axis_size("gx"), lax.axis_size("gy")
    xside = ({"gx": lax.rem(ix + nx - 1, nx)}, {"gx": lax.rem(ix + 1, nx)})
    yside = ({"gy": lax.rem(iy + ny - 1, ny)}, {"gy": lax.rem(iy + 1, ny)})
    others = [{"gz": lax.rem(me + k, tiles)} for k in range(1, tiles)]
    has_low, has_high = me > 0, me < tiles - 1
    relays = nx == 8
    ax4 = lax.rem(ix, 4)
    far = (ax4 == 0, ax4 == 3) if relays else (ix < 0, ix < 0)
    relaying = (ax4 == 1, ax4 == 2)
    across = 6 + 2 * lax.rem(ix, 2) - ix
    zside = ({"gz": jnp.maximum(me - 1, 0)}, {"gz": jnp.minimum(me + 1, tiles - 1)})
    has = (has_low, has_high)

    bring = [
        pltpu.make_async_copy(slots, lists_in.at[0], loads.at[0]),
        pltpu.make_async_copy(owners, lists_in.at[1], loads.at[1]),
        pltpu.make_async_copy(offsets, lists_in.at[2:5], loads.at[2]),
        pltpu.make_async_copy(grains, ext.at[0:12, 3:11, 0:16], loads.at[3]),
        pltpu.make_async_copy(solute, ext.at[SOL, 3:11, 0:16], loads.at[4]),
        pltpu.make_async_copy(thermal, stored, loads.at[5]),
    ]
    for c in bring:
        c.start()

    barrier = pltpu.get_barrier_semaphore()
    xy = [[{**xside[s], **yside[t]} for s in range(2)] for t in range(2)]
    xz = [[{**xside[s], **zside[d]} for s in range(2)] for d in range(2)]
    yz = [[{**yside[t], **zside[d]} for d in range(2)] for t in range(2)]
    partners = [*xside, *yside, *others, *xy[0], *xy[1]]
    if relays:
        partners.append({"gx": across})
    for d in partners:
        pl.semaphore_signal(barrier, inc=1, device_id=d, device_id_type=MESH)
    for d in range(2):
        @pl.when(has[d])
        def _(d=d):
            for p in (*xz[d], yz[0][d], yz[1][d]):
                pl.semaphore_signal(barrier, inc=1, device_id=p, device_id_type=MESH)

    def remote(src, dst, ss, rs, d):
        return pltpu.make_async_remote_copy(
            src_ref=src, dst_ref=dst, send_sem=ss, recv_sem=rs, device_id=d, device_id_type=MESH
        )

    for c in bring[0:3]:
        c.wait()
    live = lists_in[1] >= 0
    livef = live.astype(F32)
    off = [lists_in[2 + i] for i in range(3)]
    req[...] = jnp.zeros((8, 128), F32)
    req[KEY : KEY + 1, 0:20] = jnp.where(live, lists_in[1] * 64 + lists_in[0], -1).astype(F32)
    for i in range(3):
        req[HZ + i : HZ + i + 1, 0:20] = ((off[i] + (off[i] & 1)) >> 1).astype(F32) * livef
    req[LIVE : LIVE + 1, 0:20] = livef
    req[TILE : TILE + 1, 0:20] = livef * me.astype(F32)

    for c in bring[3:5]:
        c.wait()
    for s, first in ((0, 0), (1, 13)):
        def pack(f, _, s=s, first=first):
            for i in range(3):
                xp[s, f, i * 8 : i * 8 + 8, :] = ext[f, 3:11, first + i, :]
            return 0
        lax.fori_loop(0, 13, pack, 0)

    pl.semaphore_wait(barrier, len(partners) + 4 * (jnp.minimum(me, 1) + jnp.minimum(tiles - 1 - me, 1)))

    request = [
        remote(req, rq.at[me], s_rq.at[k], r_rq.at[me], d) for k, d in enumerate(others)
    ]
    for c in request:
        c.start()
    xcopy = []
    for s in range(2):
        xcopy.append(remote(xp.at[s, 0:DIRECT], xr.at[1 - s, 0:DIRECT], s_x.at[s], r_x.at[1 - s], xside[s]))
    for s in range(2):
        xcopy.append(remote(
            xp.at[s, DIRECT:13], xr.at[1 - s, DIRECT:13], s_x.at[2 + s], r_x.at[3 - s], xside[s]
        ))
    by_way = [remote(xp.at[s, DIRECT:13], relay, s_x.at[2 + s], r_relay, xside[1 - s]) for s in range(2)]
    onward = [
        remote(relay, xr.at[1 - s, DIRECT:13], s_relay, r_x.at[3 - s], {"gx": across}) for s in range(2)
    ]
    if relays:
        for s in range(2):
            @pl.when(far[s])
            def _(s=s):
                by_way[s].start()
    for s in range(2):
        xcopy[s].start()
    for s in range(2):
        @pl.when(jnp.logical_not(far[s]))
        def _(s=s):
            xcopy[2 + s].start()
    zrows = ((0, 11), (5, 0))
    zcopy = []
    for d in range(2):
        a, b = zrows[d]
        zcopy.append(remote(
            ext.at[0:13, 3 + a : 6 + a, 0:16], ext.at[0:13, b : b + 3, 0:16], s_z.at[d], r_z.at[d], zside[d]
        ))

        @pl.when(has[d])
        def _(d=d):
            zcopy[d].start()

    row8, lane8 = iota((8, 128), 0), iota((8, 128), 1) >> 4
    bring[5].wait()

    def turn(g, _):
        rows = pl.ds(pl.multiple_of(g * 8, 8), 8)
        for c in range(32):
            v = stored[rows, c * 128 : c * 128 + 128]
            for k in (1, 2, 4):
                rb, lbit = (row8 & k) != 0, (lane8 & k) != 0
                a = pltpu.roll(pltpu.roll(v, 8 - k, 0), 16 * k, 1)
                b = pltpu.roll(pltpu.roll(v, k, 0), 128 - 16 * k, 1)
                v = jnp.where(rb == lbit, v, jnp.where(lbit, a, b))
            lb[g, c // 2, (c % 2) * 8 : (c % 2) * 8 + 8, :] = v
        return 0
    lax.fori_loop(0, 5, turn, 0)
    rq[me] = req[...]
    xs[...] = jnp.zeros(xs.shape, F32)

    for k in range(1, tiles):
        src = lax.rem(me + tiles - k, tiles)
        remote(req, rq.at[src], s_rq.at[k - 1], r_rq.at[src], others[k - 1]).wait_recv()

    if relays:
        for s in range(2):
            @pl.when(relaying[s])
            def _(s=s):
                by_way[s].wait_recv()
                onward[s].start()

    lists = [jnp.zeros((8, 128), F32), jnp.zeros((8, 128), F32)]
    for t in range(tiles):
        v = rq[t]
        lists[t // 4] = lists[t // 4] + (pltpu.roll(v, 32 * (t % 4), 1) if t % 4 else v)
    for h in range(2):
        prm[5 + h] = lists[h]
    base = me * 64
    for g in range(5):
        slot_of = base + g * 8 + (iota((128, 128), 0) >> 4)
        total = jnp.zeros((8, 128), F32)
        for h in range(2):
            match = jnp.where(lists[h][KEY : KEY + 1, :] == slot_of.astype(F32), 1.0, 0.0).astype(BF16)
            total = total + nt(lists[h].astype(BF16), match)
        prm[g] = total

    def choose(g, _):
        v = prm[g]
        hz, hx = v[HZ : HZ + 1, :], v[HX : HX + 1, :]
        layers = [jnp.zeros((16, 128), F32) for _ in range(5)]
        for p in range(16):
            part = lb[g, p]
            for a in range(5):
                layers[a] = layers[a] + jnp.where(hz == float(a - p), part, 0.0)
        at = iota((16, 128), 0).astype(F32) + hx
        lanes = pl.ds(pl.multiple_of(g * 128, 128), 128)
        for a in range(5):
            for b in range(AX):
                xs[a * AX + b : a * AX + b + 1, lanes] = jnp.sum(
                    jnp.where(at == float(b), layers[a], 0.0), axis=0, keepdims=True
                )
        return 0
    lax.fori_loop(0, 5, choose, 0)

    hi, lo = split(xs[...])
    both = jnp.concatenate([hi, lo], axis=0)
    where_to = []
    for g in range(5):
        v = prm[g]
        spot = v[HY : HY + 1, :] + 128.0 * v[TILE : TILE + 1, :] + (iota((1, 128), 1) & 15).astype(F32)
        where_to.append(jnp.where(v[LIVE : LIVE + 1, :] > 0.5, spot, -4096.0))
    where_to = jnp.concatenate(where_to, axis=1)
    answer = []
    for k in range(tiles - 1, -1, -1):
        t = lax.rem(me + k, tiles)
        line = (iota((128, 640), 0) + t * 128).astype(F32)
        onto = jnp.where(line == where_to, 1.0, 0.0).astype(BF16)
        out = nt(both, onto)
        gr[t] = out[0:NODES] + out[NODES : 2 * NODES]
        if k:
            c = remote(gr.at[t], gx.at[me], s_gx.at[k - 1], r_gx.at[me], others[k - 1])
            c.start()
            answer.append(c)

    def mirror(fields, rows):
        for d in range(2):
            @pl.when(jnp.logical_not(has[1 - d]))
            def _(d=d):
                def one(f, _):
                    for i in range(3):
                        if d:
                            ext[f, 2 - i, rows] = ext[f, 3 + i, rows]
                        else:
                            ext[f, 11 + i, rows] = ext[f, 10 - i, rows]
                    return 0
                lax.fori_loop(*fields, one, 0)

    for d in range(2):
        @pl.when(has[1 - d])
        def _(d=d):
            zcopy[d].wait_recv()
    inner, outer = slice(0, 16), slice(16, 24)
    mirror((0, 13), inner)

    def pack_y(rows, count):
        slot = iota((count, 128), 1) >> 3
        def one(f, _):
            v = jnp.zeros((count, 128), F32)
            for r in range(14):
                v = jnp.where(slot == r, pltpu.roll(ext[f, r, rows], r * 8 + 4, 1), v)
            pk[f, rows] = v
            return 0
        lax.fori_loop(0, 13, one, 0)

    def y_copies(rows, k):
        return [
            remote(pk.at[:, rows], yr.at[1, :, rows], s_y.at[k], r_y.at[k + 1], yside[0]),
            remote(pk.at[:, rows], yr.at[0, :, rows], s_y.at[k + 1], r_y.at[k], yside[1]),
        ]

    def unpack_y(rows, count):
        upper = (iota((count, 128), 1) & 7) >= 4
        def one(f, _):
            own = pk[f, rows]
            ext[f, LOW, rows] = jnp.where(upper, own, yr[0, f, rows])
            ext[f, HIGH, rows] = jnp.where(upper, yr[1, f, rows], own)
            return 0
        lax.fori_loop(0, 13, one, 0)

    pack_y(inner, 16)
    yinner = y_copies(inner, 0)
    for c in yinner:
        c.start()

    def unpack_x(f):
        for z in range(8):
            ext[f, 3 + z, 16:19, :] = xr[1, f, pl.ds(z, 3, stride=8), :]
            ext[f, 3 + z, 21:24, :] = xr[0, f, pl.ds(z, 3, stride=8), :]

    bz, bx, by = [
        jnp.max(jnp.where(live, o & 1, 0).astype(F32), axis=1, keepdims=True) for o in off
    ]
    node, cell = iota((128, 128), 0), iota((128, 128), 1).astype(F32)
    wy = jnp.maximum(0.0, 1.0 - jnp.abs(cell - (2.0 * node.astype(F32) - by)) * 0.5)
    wy = jnp.where(node <= 64, wy, 0.0).astype(BF16)
    ci, ki = iota((128, NODES), 0), iota((128, NODES), 1)
    az = (ki * 57) >> 9
    ax = ki - AX * az
    wz = jnp.maximum(0.0, 1.0 - jnp.abs((ci >> 4).astype(F32) - (2.0 * az.astype(F32) - bz)) * 0.5)
    wx = jnp.maximum(0.0, 1.0 - jnp.abs((ci & 15).astype(F32) - (2.0 * ax.astype(F32) - bx)) * 0.5)
    wzx = (wz * wx).astype(BF16)

    grid = gr[me]
    for k in range(1, tiles):
        src = lax.rem(me + tiles - k, tiles)
        remote(gr.at[src], gx.at[src], s_gx.at[k - 1], r_gx.at[src], others[k - 1]).wait_recv()
        grid = grid + gx[src]
    hi, lo = split(grid)
    fine = jnp.dot(jnp.concatenate([hi, lo], axis=0), wy, preferred_element_type=F32)
    fine = fine[0:NODES] + fine[NODES : 2 * NODES]
    hi, lo = split(fine)
    heat = jnp.dot(wzx, hi, preferred_element_type=F32) + jnp.dot(wzx, lo, preferred_element_type=F32)
    heat = heat.reshape(8, 16, 128)
    heat_out[...] = heat
    for z in range(8):
        ext[HEAT, 3 + z, 0:16, :] = heat[z]
    for s, first in ((0, 0), (1, 13)):
        for i in range(3):
            xp[s, HEAT, i * 8 : i * 8 + 8, :] = heat[:, first + i, :]
    xheat = [
        remote(xp.at[0, HEAT], xr.at[1, HEAT], s_xt.at[0], r_xt.at[1], xside[0]),
        remote(xp.at[1, HEAT], xr.at[0, HEAT], s_xt.at[1], r_xt.at[0], xside[1]),
    ]
    for c in xheat:
        c.start()
    zheat = []
    for d in range(2):
        a, b = zrows[d]
        zheat.append(remote(
            ext.at[HEAT, 3 + a : 6 + a, 0:16], ext.at[HEAT, b : b + 3, 0:16], s_zt.at[d], r_zt.at[d], zside[d]
        ))

        @pl.when(has[d])
        def _(d=d):
            zheat[d].start()

    for z in range(8):
        v = pltpu.roll(heat[z], (z + 3) * 8 + 4, 1)
        strips = v if z == 0 else jnp.where((iota((16, 128), 1) >> 3) == z + 3, v, strips)
    hk[...] = strips
    yheat, xyheat, xzheat, yzheat = [], [], [], []
    for t in range(2):
        yheat.append(remote(hk, hy.at[1 - t], s_hy.at[t], r_hy.at[1 - t], yside[t]))
        for s in range(2):
            n = 2 * (1 - t) + 1 - s
            xyheat.append(remote(
                hk.at[8 * s : 8 * s + 8], hxy.at[n], s_hxy.at[2 * t + s], r_hxy.at[n], xy[t][s]
            ))
    for c in (*xyheat, *yheat):
        c.start()
    for d in range(2):
        for s in range(2):
            n = 2 * d + 1 - s
            xzheat.append(remote(
                ext.at[HEAT, (3, 10)[d], 8 * s : 8 * s + 8], hxz.at[n], s_hxz.at[2 * d + s], r_hxz.at[n], xz[d][s]
            ))
        for t in range(2):
            n = 2 * d + 1 - t
            yzheat.append(remote(hk, hyz.at[n], s_hyz.at[2 * d + t], r_hyz.at[n], yz[t][d]))

        @pl.when(has[d])
        def _(d=d):
            for k in (2 * d, 2 * d + 1):
                xzheat[k].start()
                yzheat[k].start()

    for c in yinner:
        c.wait_recv()
    unpack_y(inner, 16)

    for c in xcopy:
        c.wait_recv()

    order = ((2, 1), (0, 1))
    shown = ((0, 1), (7, 6))
    dcopy = []
    for d in range(2):
        for s in range(2):
            near, far = order[s]
            z1, z2 = shown[d]
            for k, (i, z) in enumerate(((near, z1), (near, z2), (far, z1))):
                for f in range(13):
                    dp[2 * d + s, k, f : f + 1, :] = xr[s, f, i * 8 + z : i * 8 + z + 1, :]
            dcopy.append(remote(
                dp.at[2 * d + s], dr.at[2 * d + s], s_d.at[2 * d + s], r_d.at[2 * d + s], zside[d]
            ))

        @pl.when(has[d])
        def _(d=d):
            for s in range(2):
                dcopy[2 * d + s].start()

    def unpack_all(f, _):
        unpack_x(f)
        return 0
    lax.fori_loop(0, 13, unpack_all, 0)

    for d in range(2):
        @pl.when(has[1 - d])
        def _(d=d):
            for s in range(2):
                dcopy[2 * d + s].wait_recv()
            e1, e2 = ((11, 12), (2, 1))[d]
            for s in range(2):
                x1, x2 = ((23, 22), (16, 17))[s]
                for k, (e, x) in enumerate(((e1, x1), (e2, x1), (e1, x2))):
                    for f in range(13):
                        ext[f, e, x : x + 1, :] = dr[2 * d + s, k, f : f + 1, :]
    mirror((0, 13), outer)

    pack_y(outer, 8)
    youter = y_copies(outer, 2)
    for c in youter:
        c.start()

    for c in (*xheat, *yheat):
        c.wait_recv()
    for c in xyheat:
        c.wait_recv()
    unpack_x(HEAT)
    lane16, slot16, row8 = iota((16, 128), 1), iota((16, 128), 1) >> 3, iota((8, 128), 0)
    theirs = ((lane16 & 7) < 4, (lane16 & 7) >= 4)
    for p in range(2):
        ext[HEAT, LOW + p, inner] = jnp.where(theirs[p], hy[p], strips)
        ext[HEAT, LOW + p, outer] = jnp.where(row8 < 4, hxy[2 * p + 1], hxy[2 * p])
    mirror((HEAT, HEAT + 1), slice(0, 24))
    for d in range(2):
        new = (11, 2)[d]

        @pl.when(has[1 - d])
        def _(d=d, new=new):
            zheat[d].wait_recv()
            for k in (2 * d, 2 * d + 1):
                xzheat[k].wait_recv()
                yzheat[k].wait_recv()
            ext[HEAT, new, outer] = jnp.where(row8 < 4, hxz[2 * d + 1], hxz[2 * d])
            for p in range(2):
                ext[HEAT, LOW + p, inner] = jnp.where(
                    theirs[p] & (slot16 == new), pltpu.roll(hyz[2 * d + p], 64, 1), ext[HEAT, LOW + p, inner]
                )

        @pl.when(jnp.logical_not(has[1 - d]))
        def _(d=d, new=new):
            for p in range(2):
                v = ext[HEAT, LOW + p, inner]
                ext[HEAT, LOW + p, inner] = jnp.where(
                    theirs[p] & (slot16 == new), pltpu.roll(v, (8, 120)[d], 1), v
                )

    for c in youter:
        c.wait_recv()
    unpack_y(outer, 8)

    def step(src, dst, first, last):
        def sums(r, _):
            s = src[0, r] * src[0, r]
            for f in range(1, 12):
                s = s + src[f, r] * src[f, r]
            u = src[SOL, r]
            squares[r] = s
            bend[r] = u - 0.5 * s
            drives[r] = 60.0 * (1.0 - ext[HEAT, r] - 0.5 * u)
            return 0
        lax.fori_loop(0, 16, sums, 0)
        final = dst is None
        n = 16 if final else 24

        def fields(f, _):
            low, high = src[f, LOW], src[f, HIGH]
            edge = edges(low, high)[0:n]
            for r in range(first, last):
                c = src[f, r]
                around = main_neighbours(src[f, r - 1, 0:n], c, src[f, r + 1, 0:n], edge, r)
                v = grown(c[0:n], around, squares[r, 0:n], drives[r, 0:n])
                if final:
                    grains_out[f, r - 3] = v
                else:
                    dst[f, r] = v
            if not final:
                for r, c in ((LOW, low), (HIGH, high)):
                    dst[f, r] = grown(c, strip_neighbours(c), squares[r], drives[r])
            return 0
        lax.fori_loop(0, 12, fields, 0)
        low, high = bend[LOW], bend[HIGH]
        edge = edges(low, high)[0:n]
        for r in range(first, last):
            c = bend[r]
            lap = main_neighbours(bend[r - 1, 0:n], c, bend[r + 1, 0:n], edge, r) - 6.0 * c[0:n]
            v = src[SOL, r, 0:n] + 0.15 * lap
            if final:
                solute_out[r - 3] = v
            else:
                dst[SOL, r] = v
        if not final:
            for r, c in ((LOW, low), (HIGH, high)):
                dst[SOL, r] = src[SOL, r] + 0.15 * (strip_neighbours(c) - 6.0 * c)

    step(ext, alt, 1, 13)
    for d in range(2):
        @pl.when(has[d])
        def _(d=d):
            zcopy[d].wait_send()

    step(alt, ext, 2, 12)
    step(ext, None, 3, 11)

    for c in [*request, *xcopy, *answer, *xheat, *yinner, *youter, *yheat, *xyheat]:
        c.wait_send()
    for d in range(2):
        @pl.when(has[d])
        def _(d=d):
            for k in (2 * d, 2 * d + 1):
                for c in (dcopy[k], xzheat[k], yzheat[k]):
                    c.wait_send()
            zheat[d].wait_send()
    if relays:
        @pl.when(relaying[0] | relaying[1])
        def _():
            onward[0].wait_send()


def body(grains, solute, thermal, block_slot, block_owner, block_offset):
    tiles = lax.axis_size("gz")
    vmem = pl.BlockSpec(memory_space=pltpu.VMEM)
    dma = pltpu.SemaphoreType.DMA
    import functools

    return pl.pallas_call(
        functools.partial(kernel, tiles),
        out_shape=(
            jax.ShapeDtypeStruct(grains.shape, F32),
            jax.ShapeDtypeStruct(solute.shape, F32),
            jax.ShapeDtypeStruct(solute.shape, F32),
        ),
        in_specs=[pl.BlockSpec(memory_space=pltpu.HBM)] * 6,
        out_specs=(vmem,) * 3,
        scratch_shapes=[
            pltpu.VMEM((NF, 16, 24, 128), F32),
            pltpu.VMEM((13, 16, 24, 128), F32),
            pltpu.VMEM((16, 24, 128), F32),
            pltpu.VMEM((16, 24, 128), F32),
            pltpu.VMEM((16, 24, 128), F32),
            pltpu.VMEM((2, NF, 24, 128), F32),
            pltpu.VMEM((2, NF, 24, 128), F32),
            pltpu.VMEM((13 - DIRECT, 24, 128), F32),
            pltpu.VMEM((4, 3, 16, 128), F32),
            pltpu.VMEM((4, 3, 16, 128), F32),
            pltpu.VMEM((13, 24, 128), F32),
            pltpu.VMEM((2, 13, 24, 128), F32),
            pltpu.VMEM((16, 128), F32),
            pltpu.VMEM((2, 16, 128), F32),
            pltpu.VMEM((4, 8, 128), F32),
            pltpu.VMEM((4, 8, 128), F32),
            pltpu.VMEM((4, 16, 128), F32),
            pltpu.VMEM((40, 4096), F32),
            pltpu.VMEM((5, 1, 20), jnp.int32),
            pltpu.VMEM((8, 128), F32),
            pltpu.VMEM((tiles, 8, 128), F32),
            pltpu.VMEM((5, 16, 16, 128), F32),
            pltpu.VMEM((7, 8, 128), F32),
            pltpu.VMEM((NODES, 640), F32),
            pltpu.VMEM((tiles, NODES, 128), F32),
            pltpu.VMEM((tiles, NODES, 128), F32),
            dma((6,)), dma((tiles,)), dma((tiles,)), dma((tiles,)), dma((tiles,)),
            dma((2,)), dma((2,)), dma((4,)), dma((4,)),
            dma((2,)), dma((2,)), dma((2,)), dma((2,)),
            dma((4,)), dma((4,)), dma((4,)), dma((4,)),
            dma, dma, dma((2,)), dma((2,)), dma((4,)), dma((4,)),
            dma((4,)), dma((4,)), dma((4,)), dma((4,)),
        ],
        compiler_params=pltpu.CompilerParams(
            collective_id=0, has_side_effects=True, vmem_limit_bytes=66000000
        ),
    )(
        grains,
        solute,
        thermal.reshape(thermal.shape[3], thermal.shape[4]),
        block_slot.reshape(1, -1),
        block_owner.reshape(1, -1),
        block_offset.reshape(3, 1, -1),
    )


def solution(mesh):
    in_specs = (
        P(None, "gz", "gx", "gy"),
        P("gz", "gx", "gy"),
        P("gz", "gx", "gy", None, None),
        P("gz", "gx", "gy", None),
        P("gz", "gx", "gy", None),
        P("gz", "gx", "gy", None, None),
    )
    out_specs = (P(None, "gz", "gx", "gy"), P("gz", "gx", "gy"), P("gz", "gx", "gy"))
    return jax.shard_map(body, mesh=mesh, in_specs=in_specs, out_specs=out_specs, check_vma=False)
```

```python
import jax
import jax.numpy as jnp
from jax import lax
from jax.experimental import pallas as pl
from jax.experimental.pallas import tpu as pltpu
from jax.sharding import PartitionSpec as P

F32 = jnp.float32
BF16 = jnp.bfloat16
MESH = pl.DeviceIdType.MESH
NF = 14
SOL = 12
HEAT = 13
DIRECT = 4
EARLY = 7
KEY, HZ, HX, HY, LIVE, TILE = range(6)
AX = 9
NODES = 48
LOW, HIGH = 14, 15


def iota(shape, axis):
    return lax.broadcasted_iota(jnp.int32, shape, axis)


def split(x):
    high = x.astype(BF16)
    return high, (x - high.astype(F32)).astype(BF16)


def nt(a, b):
    return lax.dot_general(a, b, (((1,), (1,)), ((), ())), preferred_element_type=F32)


GROUPS = ((8, 16), (16, 24), (0, 8))


def edges(low, high):
    return jnp.where((iota(low.shape, 1) & 7) == 3, low, pltpu.roll(high, 126, 1))


def along_x(ref, r, a):
    sub = iota((8, 128), 0)
    if a == 0:
        before = jnp.where(sub == 0, ref[r, 23:24, :], pltpu.roll(ref[r, 0:8, :], 1, 0))
        return before + ref[r, 1:9, :]
    after = ref[r, a + 1 : a + 9, :]
    if a == 16:
        after = jnp.where(sub == 7, ref[r, 0:1, :], after)
    return ref[r, a - 1 : a + 7, :] + after


def main_neighbours(ref, r, a, edge):
    lane = iota((8, 128), 1)
    c = ref[r, a : a + 8, :]
    beyond = pltpu.roll(edge, (125 - r * 8) % 128, 1)
    left = jnp.where(lane == 0, beyond, pltpu.roll(c, 1, 1))
    right = jnp.where(lane == 127, beyond, pltpu.roll(c, 127, 1))
    return c, (ref[r - 1, a : a + 8, :] + ref[r + 1, a : a + 8, :]) + along_x(ref, r, a) + (left + right)


def strip_neighbours(ref, r, a):
    c = ref[r, a : a + 8, :]
    z = pltpu.roll(c, 8, 1) + pltpu.roll(c, 120, 1)
    y = pltpu.roll(c, 1, 1) + pltpu.roll(c, 127, 1)
    return c, z + y + along_x(ref, r, a)


def grown(c, around, s, drive):
    cc = c * c
    w = c - cc
    return w * ((0.4 * c - 0.2) + w * drive) + c * (0.1 * cc - s) + 0.16 * around


def kernel(
    tiles,
    grains, solute, thermal, slots, owners, offsets,
    grains_out, solute_out, heat_out,
    ext, alt, bend, squares, drives,
    xp, xr, relay, dp, dr, pk, yr,
    hk, hy, hxz, hxy, hyz,
    stored, lists_in, req, rq, lb, prm, xs, gr, gx,
    loads, s_rq, r_rq, s_gx, r_gx, s_z, r_z, s_x, r_x, s_zt, r_zt, s_xt, r_xt, s_d, r_d, s_y, r_y,
    s_relay, r_relay, s_hy, r_hy, s_hxz, r_hxz, s_hxy, r_hxy, s_hyz, r_hyz,
):
    me = lax.axis_index("gz")
    ix, iy = lax.axis_index("gx"), lax.axis_index("gy")
    nx, ny = lax.axis_size("gx"), lax.axis_size("gy")
    xside = ({"gx": lax.rem(ix + nx - 1, nx)}, {"gx": lax.rem(ix + 1, nx)})
    yside = ({"gy": lax.rem(iy + ny - 1, ny)}, {"gy": lax.rem(iy + 1, ny)})
    others = [{"gz": lax.rem(me + k, tiles)} for k in range(1, tiles)]
    has_low, has_high = me > 0, me < tiles - 1
    relays = nx == 8
    ax4 = lax.rem(ix, 4)
    far = (ax4 == 0, ax4 == 3) if relays else (ix < 0, ix < 0)
    relaying = (ax4 == 1, ax4 == 2)
    across = 6 + 2 * lax.rem(ix, 2) - ix
    zside = ({"gz": jnp.maximum(me - 1, 0)}, {"gz": jnp.minimum(me + 1, tiles - 1)})
    has = (has_low, has_high)

    bring = [
        pltpu.make_async_copy(slots, lists_in.at[0], loads.at[0]),
        pltpu.make_async_copy(owners, lists_in.at[1], loads.at[1]),
        pltpu.make_async_copy(offsets, lists_in.at[2:5], loads.at[2]),
        pltpu.make_async_copy(grains, ext.at[0:12, 3:11, 8:24], loads.at[3]),
        pltpu.make_async_copy(solute, ext.at[SOL, 3:11, 8:24], loads.at[4]),
        pltpu.make_async_copy(thermal, stored, loads.at[5]),
    ]
    for c in bring:
        c.start()

    barrier = pltpu.get_barrier_semaphore()
    xy = [[{**xside[s], **yside[t]} for s in range(2)] for t in range(2)]
    xz = [[{**xside[s], **zside[d]} for s in range(2)] for d in range(2)]
    yz = [[{**yside[t], **zside[d]} for d in range(2)] for t in range(2)]
    partners = [*xside, *yside, *others, *xy[0], *xy[1]]
    if relays:
        partners.append({"gx": across})
    for d in partners:
        pl.semaphore_signal(barrier, inc=1, device_id=d, device_id_type=MESH)
    for d in range(2):
        @pl.when(has[d])
        def _(d=d):
            for p in (*xz[d], yz[0][d], yz[1][d]):
                pl.semaphore_signal(barrier, inc=1, device_id=p, device_id_type=MESH)

    def remote(src, dst, ss, rs, d):
        return pltpu.make_async_remote_copy(
            src_ref=src, dst_ref=dst, send_sem=ss, recv_sem=rs, device_id=d, device_id_type=MESH
        )

    for c in bring[0:3]:
        c.wait()
    live = lists_in[1] >= 0
    livef = live.astype(F32)
    off = [lists_in[2 + i] for i in range(3)]
    req[...] = jnp.zeros((8, 128), F32)
    req[KEY : KEY + 1, 0:20] = jnp.where(live, lists_in[1] * 64 + lists_in[0], -1).astype(F32)
    for i in range(3):
        req[HZ + i : HZ + i + 1, 0:20] = ((off[i] + (off[i] & 1)) >> 1).astype(F32) * livef
    req[LIVE : LIVE + 1, 0:20] = livef
    req[TILE : TILE + 1, 0:20] = livef * me.astype(F32)

    for c in bring[3:5]:
        c.wait()
    for s, first in ((0, 0), (1, 13)):
        def pack(f, _, s=s, first=first):
            for i in range(3):
                xp[s, f, i * 8 : i * 8 + 8, :] = ext[f, 3:11, 8 + first + i, :]
            return 0
        lax.fori_loop(0, 13, pack, 0)

    pl.semaphore_wait(barrier, len(partners) + 4 * (jnp.minimum(me, 1) + jnp.minimum(tiles - 1 - me, 1)))

    request = [
        remote(req, rq.at[me], s_rq.at[k], r_rq.at[me], d) for k, d in enumerate(others)
    ]
    for c in request:
        c.start()
    xcopy = []
    for s in range(2):
        xcopy.append(remote(xp.at[s, 0:DIRECT], xr.at[1 - s, 0:DIRECT], s_x.at[s], r_x.at[1 - s], xside[s]))
    for s in range(2):
        xcopy.append(remote(
            xp.at[s, DIRECT:13], xr.at[1 - s, DIRECT:13], s_x.at[2 + s], r_x.at[3 - s], xside[s]
        ))
    by_way = [remote(xp.at[s, DIRECT:13], relay, s_x.at[2 + s], r_relay, xside[1 - s]) for s in range(2)]
    onward = [
        remote(relay, xr.at[1 - s, DIRECT:13], s_relay, r_x.at[3 - s], {"gx": across}) for s in range(2)
    ]
    if relays:
        for s in range(2):
            @pl.when(far[s])
            def _(s=s):
                by_way[s].start()
    for s in range(2):
        xcopy[s].start()
    for s in range(2):
        @pl.when(jnp.logical_not(far[s]))
        def _(s=s):
            xcopy[2 + s].start()
    zrows = ((0, 11), (5, 0))
    zcopy = []
    for d in range(2):
        a, b = zrows[d]
        zcopy.append([
            remote(
                ext.at[f, 3 + a : 6 + a, 8:24], ext.at[f, b : b + 3, 8:24], s_z.at[2 * k + d], r_z.at[2 * k + d], zside[d]
            )
            for k, f in enumerate((slice(0, EARLY), slice(EARLY, 13)))
        ])

        @pl.when(has[d])
        def _(d=d):
            zcopy[d][0].start()


    row8, lane8 = iota((8, 128), 0), iota((8, 128), 1) >> 4
    bring[5].wait()

    def turn(g, _):
        rows = pl.ds(pl.multiple_of(g * 8, 8), 8)
        for c in range(32):
            v = stored[rows, c * 128 : c * 128 + 128]
            for k in (1, 2, 4):
                rb, lbit = (row8 & k) != 0, (lane8 & k) != 0
                a = pltpu.roll(pltpu.roll(v, 8 - k, 0), 16 * k, 1)
                b = pltpu.roll(pltpu.roll(v, k, 0), 128 - 16 * k, 1)
                v = jnp.where(rb == lbit, v, jnp.where(lbit, a, b))
            lb[g, c // 2, (c % 2) * 8 : (c % 2) * 8 + 8, :] = v
        return 0
    lax.fori_loop(0, 5, turn, 0)
    rq[me] = req[...]
    xs[...] = jnp.zeros(xs.shape, F32)

    for k in range(1, tiles):
        src = lax.rem(me + tiles - k, tiles)
        remote(req, rq.at[src], s_rq.at[k - 1], r_rq.at[src], others[k - 1]).wait_recv()

    if relays:
        for s in range(2):
            @pl.when(relaying[s])
            def _(s=s):
                by_way[s].wait_recv()
                onward[s].start()

    lists = [jnp.zeros((8, 128), F32), jnp.zeros((8, 128), F32)]
    for t in range(tiles):
        v = rq[t]
        lists[t // 4] = lists[t // 4] + (pltpu.roll(v, 32 * (t % 4), 1) if t % 4 else v)
    for h in range(2):
        prm[5 + h] = lists[h]
    base = me * 64
    for g in range(5):
        slot_of = base + g * 8 + (iota((128, 128), 0) >> 4)
        total = jnp.zeros((8, 128), F32)
        for h in range(2):
            match = jnp.where(lists[h][KEY : KEY + 1, :] == slot_of.astype(F32), 1.0, 0.0).astype(BF16)
            total = total + nt(lists[h].astype(BF16), match)
        prm[g] = total

    def choose(g, _):
        v = prm[g]
        hz, hx = v[HZ : HZ + 1, :], v[HX : HX + 1, :]
        layers = [jnp.zeros((16, 128), F32) for _ in range(5)]
        for p in range(16):
            part = lb[g, p]
            for a in range(5):
                layers[a] = layers[a] + jnp.where(hz == float(a - p), part, 0.0)
        at = iota((16, 128), 0).astype(F32) + hx
        lanes = pl.ds(pl.multiple_of(g * 128, 128), 128)
        for a in range(5):
            for b in range(AX):
                xs[a * AX + b : a * AX + b + 1, lanes] = jnp.sum(
                    jnp.where(at == float(b), layers[a], 0.0), axis=0, keepdims=True
                )
        return 0
    lax.fori_loop(0, 5, choose, 0)

    hi, lo = split(xs[...])
    both = jnp.concatenate([hi, lo], axis=0)
    where_to = []
    for g in range(5):
        v = prm[g]
        spot = v[HY : HY + 1, :] + 128.0 * v[TILE : TILE + 1, :] + (iota((1, 128), 1) & 15).astype(F32)
        where_to.append(jnp.where(v[LIVE : LIVE + 1, :] > 0.5, spot, -4096.0))
    where_to = jnp.concatenate(where_to, axis=1)
    tile_of = lax.rem(me + iota((8, 640), 0), tiles) * 128 + 64
    last = jnp.where(tile_of.astype(F32) == where_to, 1.0, 0.0).astype(BF16)
    blank = jnp.zeros((64, 640), BF16)
    tail = nt(last, jnp.concatenate([blank, hi, blank[0:16]], axis=0))
    tail = tail + nt(last, jnp.concatenate([blank, lo, blank[0:16]], axis=0))
    lane, at_last = iota((24, 128), 1), iota((24, 128), 0) == 23
    answer = []
    for k in range(tiles - 1, -1, -1):
        t = lax.rem(me + k, tiles)
        line = (iota((128, 640), 0) + t * 128).astype(F32)
        onto = jnp.where(line == where_to, 1.0, 0.0).astype(BF16)
        out = nt(both, onto)
        out = out[0:NODES] + out[NODES : 2 * NODES]
        upper = jnp.where(at_last, tail[k : k + 1, :], pltpu.roll(out[24:48], 64, 1))
        gr[t] = jnp.where(lane < 64, out[0:24], upper)
        if k:
            c = remote(gr.at[t], gx.at[me], s_gx.at[k - 1], r_gx.at[me], others[k - 1])
            c.start()
            answer.append(c)

    for d in range(2):
        @pl.when(has[d])
        def _(d=d):
            zcopy[d][1].start()

    inner, outer = slice(8, 24), slice(0, 8)
    def mirror(fields, rows):
        for d in range(2):
            @pl.when(jnp.logical_not(has[1 - d]))
            def _(d=d):
                def one(f, _):
                    for i in range(3):
                        if d:
                            ext[f, 2 - i, rows] = ext[f, 3 + i, rows]
                        else:
                            ext[f, 11 + i, rows] = ext[f, 10 - i, rows]
                    return 0
                lax.fori_loop(*fields, one, 0)

    def pack_y(rows, count):
        slot = iota((count, 128), 1) >> 3
        def one(f, _):
            v = jnp.zeros((count, 128), F32)
            for r in range(14):
                v = jnp.where(slot == r, pltpu.roll(ext[f, r, rows], r * 8 + 4, 1), v)
            pk[f, rows] = v
            return 0
        lax.fori_loop(0, 13, one, 0)

    def y_copies(rows, k):
        return [
            remote(pk.at[:, rows], yr.at[1, :, rows], s_y.at[k], r_y.at[k + 1], yside[0]),
            remote(pk.at[:, rows], yr.at[0, :, rows], s_y.at[k + 1], r_y.at[k], yside[1]),
        ]

    def unpack_y(rows, count):
        upper = (iota((count, 128), 1) & 7) >= 4
        def one(f, _):
            own = pk[f, rows]
            ext[f, LOW, rows] = jnp.where(upper, own, yr[0, f, rows])
            ext[f, HIGH, rows] = jnp.where(upper, yr[1, f, rows], own)
            return 0
        lax.fori_loop(0, 13, one, 0)

    def unpack_x(f):
        for z in range(8):
            ext[f, 3 + z, 0:3, :] = xr[1, f, pl.ds(z, 3, stride=8), :]
            ext[f, 3 + z, 5:8, :] = xr[0, f, pl.ds(z, 3, stride=8), :]

    bz, bx, by = [
        jnp.max(jnp.where(live, o & 1, 0).astype(F32), axis=1, keepdims=True) for o in off
    ]
    node, cell = iota((128, 128), 0), iota((128, 128), 1).astype(F32)
    wy = jnp.maximum(0.0, 1.0 - jnp.abs(cell - (2.0 * node.astype(F32) - by)) * 0.5)
    wy = jnp.where(node < 64, wy, 0.0).astype(BF16)
    w64 = jnp.maximum(0.0, 1.0 - jnp.abs(iota((1, 128), 1).astype(F32) - (128.0 - by)) * 0.5)
    ci, ki = iota((128, NODES), 0), iota((128, NODES), 1)
    az = (ki * 57) >> 9
    ax = ki - AX * az
    wz = jnp.maximum(0.0, 1.0 - jnp.abs((ci >> 4).astype(F32) - (2.0 * az.astype(F32) - bz)) * 0.5)
    wx = jnp.maximum(0.0, 1.0 - jnp.abs((ci & 15).astype(F32) - (2.0 * ax.astype(F32) - bx)) * 0.5)
    wzx32 = wz * wx
    wzx = wzx32.astype(BF16)

    grid = gr[me]
    for k in range(1, tiles):
        src = lax.rem(me + tiles - k, tiles)
        remote(gr.at[src], gx.at[src], s_gx.at[k - 1], r_gx.at[src], others[k - 1]).wait_recv()
        grid = grid + gx[src]
    turned = pltpu.roll(grid, 64, 1)
    column = jnp.sum(wzx32 * turned[23:24, 0:NODES], axis=1, keepdims=True)
    hi, lo = split(jnp.concatenate([grid, turned], axis=0))
    fine = jnp.dot(jnp.concatenate([hi, lo], axis=0), wy, preferred_element_type=F32)
    fine = fine[0:NODES] + fine[NODES : 2 * NODES]
    hi, lo = split(fine)
    heat = jnp.dot(wzx, hi, preferred_element_type=F32) + jnp.dot(wzx, lo, preferred_element_type=F32)
    heat = heat + column * w64
    heat = heat.reshape(8, 16, 128)
    heat_out[...] = heat
    for z in range(8):
        ext[HEAT, 3 + z, 8:24, :] = heat[z]
    for s, first in ((0, 0), (1, 13)):
        for i in range(3):
            xp[s, HEAT, i * 8 : i * 8 + 8, :] = heat[:, first + i, :]
    xheat = [
        remote(xp.at[0, HEAT], xr.at[1, HEAT], s_xt.at[0], r_xt.at[1], xside[0]),
        remote(xp.at[1, HEAT], xr.at[0, HEAT], s_xt.at[1], r_xt.at[0], xside[1]),
    ]
    for c in xheat:
        c.start()
    zheat = []
    for d in range(2):
        a, b = zrows[d]
        zheat.append(remote(
            ext.at[HEAT, 3 + a : 6 + a, 8:24], ext.at[HEAT, b : b + 3, 8:24], s_zt.at[d], r_zt.at[d], zside[d]
        ))

        @pl.when(has[d])
        def _(d=d):
            zheat[d].start()

    for z in range(8):
        v = pltpu.roll(heat[z], (z + 3) * 8 + 4, 1)
        strips = v if z == 0 else jnp.where((iota((16, 128), 1) >> 3) == z + 3, v, strips)
    hk[...] = strips
    yheat, xyheat, xzheat, yzheat = [], [], [], []
    for t in range(2):
        yheat.append(remote(hk, hy.at[1 - t], s_hy.at[t], r_hy.at[1 - t], yside[t]))
        for s in range(2):
            n = 2 * (1 - t) + 1 - s
            xyheat.append(remote(
                hk.at[8 * s : 8 * s + 8], hxy.at[n], s_hxy.at[2 * t + s], r_hxy.at[n], xy[t][s]
            ))
    for c in (*xyheat, *yheat):
        c.start()
    for d in range(2):
        for s in range(2):
            n = 2 * d + 1 - s
            xzheat.append(remote(
                ext.at[HEAT, (3, 10)[d], 8 * s + 8 : 8 * s + 16], hxz.at[n], s_hxz.at[2 * d + s], r_hxz.at[n], xz[d][s]
            ))
        for t in range(2):
            n = 2 * d + 1 - t
            yzheat.append(remote(hk, hyz.at[n], s_hyz.at[2 * d + t], r_hyz.at[n], yz[t][d]))

        @pl.when(has[d])
        def _(d=d):
            for k in (2 * d, 2 * d + 1):
                xzheat[k].start()
                yzheat[k].start()

    for c in xcopy:
        c.wait_recv()

    order = ((2, 1), (0, 1))
    shown = ((0, 1), (7, 6))
    dcopy = []
    for d in range(2):
        for s in range(2):
            near, far = order[s]
            z1, z2 = shown[d]
            for k, (i, z) in enumerate(((near, z1), (near, z2), (far, z1))):
                for f in range(13):
                    dp[2 * d + s, k, f : f + 1, :] = xr[s, f, i * 8 + z : i * 8 + z + 1, :]
            dcopy.append(remote(
                dp.at[2 * d + s], dr.at[2 * d + s], s_d.at[2 * d + s], r_d.at[2 * d + s], zside[d]
            ))

        @pl.when(has[d])
        def _(d=d):
            for s in range(2):
                dcopy[2 * d + s].start()

    def unpack_all(f, _):
        unpack_x(f)
        return 0
    lax.fori_loop(0, 13, unpack_all, 0)

    for d in range(2):
        @pl.when(has[1 - d])
        def _(d=d):
            for s in range(2):
                dcopy[2 * d + s].wait_recv()
            e1, e2 = ((11, 12), (2, 1))[d]
            for s in range(2):
                x1, x2 = ((7, 6), (0, 1))[s]
                for k, (e, x) in enumerate(((e1, x1), (e2, x1), (e1, x2))):
                    for f in range(13):
                        ext[f, e, x : x + 1, :] = dr[2 * d + s, k, f : f + 1, :]
    mirror((0, 13), outer)

    pack_y(outer, 8)
    youter = y_copies(outer, 2)
    for c in youter:
        c.start()

    for d in range(2):
        @pl.when(has[1 - d])
        def _(d=d):
            for c in zcopy[d]:
                c.wait_recv()
    mirror((0, 13), inner)
    pack_y(inner, 16)
    yinner = y_copies(inner, 0)
    for c in yinner:
        c.start()

    for c in (*xheat, *yheat):
        c.wait_recv()
    for c in xyheat:
        c.wait_recv()
    unpack_x(HEAT)
    lane16, slot16, row8 = iota((16, 128), 1), iota((16, 128), 1) >> 3, iota((8, 128), 0)
    theirs = ((lane16 & 7) < 4, (lane16 & 7) >= 4)
    for p in range(2):
        ext[HEAT, LOW + p, inner] = jnp.where(theirs[p], hy[p], strips)
        ext[HEAT, LOW + p, outer] = jnp.where(row8 < 4, hxy[2 * p + 1], hxy[2 * p])
    mirror((HEAT, HEAT + 1), slice(0, 24))
    for d in range(2):
        new = (11, 2)[d]

        @pl.when(has[1 - d])
        def _(d=d, new=new):
            zheat[d].wait_recv()
            for k in (2 * d, 2 * d + 1):
                xzheat[k].wait_recv()
                yzheat[k].wait_recv()
            ext[HEAT, new, outer] = jnp.where(row8 < 4, hxz[2 * d + 1], hxz[2 * d])
            for p in range(2):
                ext[HEAT, LOW + p, inner] = jnp.where(
                    theirs[p] & (slot16 == new), pltpu.roll(hyz[2 * d + p], 64, 1), ext[HEAT, LOW + p, inner]
                )

        @pl.when(jnp.logical_not(has[1 - d]))
        def _(d=d, new=new):
            for p in range(2):
                v = ext[HEAT, LOW + p, inner]
                ext[HEAT, LOW + p, inner] = jnp.where(
                    theirs[p] & (slot16 == new), pltpu.roll(v, (8, 120)[d], 1), v
                )

    for c in youter:
        c.wait_recv()
    unpack_y(outer, 8)
    for c in yinner:
        c.wait_recv()
    unpack_y(inner, 16)

    def step(src, dst, first, last):
        cells = slice(0, 24)

        def sums(r, _):
            s = src[0, r, cells] * src[0, r, cells]
            for f in range(1, 12):
                s = s + src[f, r, cells] * src[f, r, cells]
            u = src[SOL, r, cells]
            squares[r] = 0.1 * s - 0.04
            bend[r, cells] = u - 0.5 * s
            drives[r] = 6.0 * (1.0 - ext[HEAT, r, cells] - 0.5 * u)
            return 0
        lax.fori_loop(0, 16, sums, 0)
        final = dst is None
        groups = GROUPS[0:2] if final else GROUPS

        def fields(f, _):
            now = src.at[f]
            for a, b in groups:
                edge = edges(now[LOW, a:b, :], now[HIGH, a:b, :])
                for r in range(first, last):
                    c, around = main_neighbours(now, r, a, edge)
                    v = grown(c, around, squares[r, a:b], drives[r, a:b])
                    if final:
                        grains_out[f, r - 3, a - 8 : b - 8, :] = v
                    else:
                        dst[f, r, a:b, :] = v
                if not final:
                    for r in (LOW, HIGH):
                        c, around = strip_neighbours(now, r, a)
                        dst[f, r, a:b, :] = grown(c, around, squares[r, a:b], drives[r, a:b])
            return 0
        lax.fori_loop(0, 12, fields, 0)
        for a, b in groups:
            edge = edges(bend[LOW, a:b, :], bend[HIGH, a:b, :])
            for r in range(first, last):
                c, around = main_neighbours(bend, r, a, edge)
                v = src[SOL, r, a:b, :] + 0.15 * (around - 6.0 * c)
                if final:
                    solute_out[r - 3, a - 8 : b - 8, :] = v
                else:
                    dst[SOL, r, a:b, :] = v
            if not final:
                for r in (LOW, HIGH):
                    c, around = strip_neighbours(bend, r, a)
                    dst[SOL, r, a:b, :] = src[SOL, r, a:b, :] + 0.15 * (around - 6.0 * c)

    step(ext, alt, 1, 13)
    for d in range(2):
        @pl.when(has[d])
        def _(d=d):
            for c in zcopy[d]:
                c.wait_send()

    step(alt, ext, 2, 12)
    step(ext, None, 3, 11)

    for c in [*request, *xcopy, *answer, *xheat, *yinner, *youter, *yheat, *xyheat]:
        c.wait_send()
    for d in range(2):
        @pl.when(has[d])
        def _(d=d):
            for k in (2 * d, 2 * d + 1):
                for c in (dcopy[k], xzheat[k], yzheat[k]):
                    c.wait_send()
            zheat[d].wait_send()
    if relays:
        @pl.when(relaying[0] | relaying[1])
        def _():
            onward[0].wait_send()


def body(grains, solute, thermal, block_slot, block_owner, block_offset):
    tiles = lax.axis_size("gz")
    vmem = pl.BlockSpec(memory_space=pltpu.VMEM)
    dma = pltpu.SemaphoreType.DMA
    import functools

    return pl.pallas_call(
        functools.partial(kernel, tiles),
        out_shape=(
            jax.ShapeDtypeStruct(grains.shape, F32),
            jax.ShapeDtypeStruct(solute.shape, F32),
            jax.ShapeDtypeStruct(solute.shape, F32),
        ),
        in_specs=[pl.BlockSpec(memory_space=pltpu.HBM)] * 6,
        out_specs=(vmem,) * 3,
        scratch_shapes=[
            pltpu.VMEM((NF, 16, 32, 128), F32),
            pltpu.VMEM((13, 16, 32, 128), F32),
            pltpu.VMEM((16, 32, 128), F32),
            pltpu.VMEM((16, 24, 128), F32),
            pltpu.VMEM((16, 24, 128), F32),
            pltpu.VMEM((2, NF, 24, 128), F32),
            pltpu.VMEM((2, NF, 24, 128), F32),
            pltpu.VMEM((13 - DIRECT, 24, 128), F32),
            pltpu.VMEM((4, 3, 16, 128), F32),
            pltpu.VMEM((4, 3, 16, 128), F32),
            pltpu.VMEM((13, 24, 128), F32),
            pltpu.VMEM((2, 13, 24, 128), F32),
            pltpu.VMEM((16, 128), F32),
            pltpu.VMEM((2, 16, 128), F32),
            pltpu.VMEM((4, 8, 128), F32),
            pltpu.VMEM((4, 8, 128), F32),
            pltpu.VMEM((4, 16, 128), F32),
            pltpu.VMEM((40, 4096), F32),
            pltpu.VMEM((5, 1, 20), jnp.int32),
            pltpu.VMEM((8, 128), F32),
            pltpu.VMEM((tiles, 8, 128), F32),
            pltpu.VMEM((5, 16, 16, 128), F32),
            pltpu.VMEM((7, 8, 128), F32),
            pltpu.VMEM((NODES, 640), F32),
            pltpu.VMEM((tiles, 24, 128), F32),
            pltpu.VMEM((tiles, 24, 128), F32),
            dma((6,)), dma((tiles,)), dma((tiles,)), dma((tiles,)), dma((tiles,)),
            dma((4,)), dma((4,)), dma((4,)), dma((4,)),
            dma((2,)), dma((2,)), dma((2,)), dma((2,)),
            dma((4,)), dma((4,)), dma((4,)), dma((4,)),
            dma, dma, dma((2,)), dma((2,)), dma((4,)), dma((4,)),
            dma((4,)), dma((4,)), dma((4,)), dma((4,)),
        ],
        compiler_params=pltpu.CompilerParams(
            collective_id=0, has_side_effects=True, vmem_limit_bytes=66000000
        ),
    )(
        grains,
        solute,
        thermal.reshape(thermal.shape[3], thermal.shape[4]),
        block_slot.reshape(1, -1),
        block_owner.reshape(1, -1),
        block_offset.reshape(3, 1, -1),
    )


def solution(mesh):
    in_specs = (
        P(None, "gz", "gx", "gy"),
        P("gz", "gx", "gy"),
        P("gz", "gx", "gy", None, None),
        P("gz", "gx", "gy", None),
        P("gz", "gx", "gy", None),
        P("gz", "gx", "gy", None, None),
    )
    out_specs = (P(None, "gz", "gx", "gy"), P("gz", "gx", "gy"), P("gz", "gx", "gy"))
    return jax.shard_map(body, mesh=mesh, in_specs=in_specs, out_specs=out_specs, check_vma=False)
```

```python
import jax
import jax.numpy as jnp
from jax import lax
from jax.experimental import pallas as pl
from jax.experimental.pallas import tpu as pltpu
from jax.sharding import PartitionSpec as P

F32 = jnp.float32
BF16 = jnp.bfloat16
MESH = pl.DeviceIdType.MESH
NF = 14
SOL = 12
HEAT = 13
DIRECT = 4
EARLY = 7
KEY, HZ, HX, HY, LIVE, TILE = range(6)
AX = 9
NODES = 48
LOW, HIGH = 14, 15


def iota(shape, axis):
    return lax.broadcasted_iota(jnp.int32, shape, axis)


def split(x):
    high = x.astype(BF16)
    return high, (x - high.astype(F32)).astype(BF16)


def nt(a, b):
    return lax.dot_general(a, b, (((1,), (1,)), ((), ())), preferred_element_type=F32)


GROUPS = ((8, 16), (16, 24), (0, 8))


def edges(low, high):
    return jnp.where((iota(low.shape, 1) & 7) == 3, low, pltpu.roll(high, 126, 1))


def along_x(ref, r, a):
    sub = iota((8, 128), 0)
    if a == 0:
        before = jnp.where(sub == 0, ref[r, 23:24, :], pltpu.roll(ref[r, 0:8, :], 1, 0))
        return before + ref[r, 1:9, :]
    after = ref[r, a + 1 : a + 9, :]
    if a == 16:
        after = jnp.where(sub == 7, ref[r, 0:1, :], after)
    return ref[r, a - 1 : a + 7, :] + after


def main_neighbours(ref, r, a, edge):
    lane = iota((8, 128), 1)
    c = ref[r, a : a + 8, :]
    beyond = pltpu.roll(edge, (125 - r * 8) % 128, 1)
    left = jnp.where(lane == 0, beyond, pltpu.roll(c, 1, 1))
    right = jnp.where(lane == 127, beyond, pltpu.roll(c, 127, 1))
    return c, (ref[r - 1, a : a + 8, :] + ref[r + 1, a : a + 8, :]) + along_x(ref, r, a) + (left + right)


def strip_neighbours(ref, r, a):
    c = ref[r, a : a + 8, :]
    z = pltpu.roll(c, 8, 1) + pltpu.roll(c, 120, 1)
    y = pltpu.roll(c, 1, 1) + pltpu.roll(c, 127, 1)
    return c, z + y + along_x(ref, r, a)


def grown(c, around, s, drive):
    cc = c * c
    w = c - cc
    return w * ((0.4 * c - 0.2) + w * drive) + c * (0.1 * cc - s) + 0.16 * around


def kernel(
    tiles,
    grains, solute, thermal, slots, owners, offsets,
    grains_out, solute_out, heat_out,
    ext, alt, bend, squares, drives,
    xp, xr, relay, dp, dr, pk, yr,
    hk, hy, hxz, hxy, hyz,
    stored, lists_in, req, rq, lb, prm, xs, gr, gx,
    loads, s_rq, r_rq, s_gx, r_gx, s_z, r_z, s_x, r_x, s_zt, r_zt, s_xt, r_xt, s_d, r_d, s_y, r_y,
    s_relay, r_relay, s_hy, r_hy, s_hxz, r_hxz, s_hxy, r_hxy, s_hyz, r_hyz,
):
    me = lax.axis_index("gz")
    ix, iy = lax.axis_index("gx"), lax.axis_index("gy")
    nx, ny = lax.axis_size("gx"), lax.axis_size("gy")
    xside = ({"gx": lax.rem(ix + nx - 1, nx)}, {"gx": lax.rem(ix + 1, nx)})
    yside = ({"gy": lax.rem(iy + ny - 1, ny)}, {"gy": lax.rem(iy + 1, ny)})
    others = [{"gz": lax.rem(me + k, tiles)} for k in range(1, tiles)]
    has_low, has_high = me > 0, me < tiles - 1
    relays = nx == 8
    ax4 = lax.rem(ix, 4)
    far = (ax4 == 0, ax4 == 3) if relays else (ix < 0, ix < 0)
    relaying = (ax4 == 1, ax4 == 2)
    across = 6 + 2 * lax.rem(ix, 2) - ix
    zside = ({"gz": jnp.maximum(me - 1, 0)}, {"gz": jnp.minimum(me + 1, tiles - 1)})
    has = (has_low, has_high)

    bring = [
        pltpu.make_async_copy(slots, lists_in.at[0], loads.at[0]),
        pltpu.make_async_copy(owners, lists_in.at[1], loads.at[1]),
        pltpu.make_async_copy(offsets, lists_in.at[2:5], loads.at[2]),
        pltpu.make_async_copy(grains, ext.at[0:12, 3:11, 8:24], loads.at[3]),
        pltpu.make_async_copy(solute, ext.at[SOL, 3:11, 8:24], loads.at[4]),
        pltpu.make_async_copy(thermal, stored, loads.at[5]),
    ]
    for c in bring:
        c.start()

    barrier = pltpu.get_barrier_semaphore()
    xy = [[{**xside[s], **yside[t]} for s in range(2)] for t in range(2)]
    xz = [[{**xside[s], **zside[d]} for s in range(2)] for d in range(2)]
    yz = [[{**yside[t], **zside[d]} for d in range(2)] for t in range(2)]
    partners = [*xside, *yside, *others, *xy[0], *xy[1]]
    if relays:
        partners.append({"gx": across})
    for d in partners:
        pl.semaphore_signal(barrier, inc=1, device_id=d, device_id_type=MESH)
    for d in range(2):
        @pl.when(has[d])
        def _(d=d):
            for p in (*xz[d], yz[0][d], yz[1][d]):
                pl.semaphore_signal(barrier, inc=1, device_id=p, device_id_type=MESH)

    def remote(src, dst, ss, rs, d):
        return pltpu.make_async_remote_copy(
            src_ref=src, dst_ref=dst, send_sem=ss, recv_sem=rs, device_id=d, device_id_type=MESH
        )

    for c in bring[0:3]:
        c.wait()
    live = lists_in[1] >= 0
    livef = live.astype(F32)
    off = [lists_in[2 + i] for i in range(3)]
    req[...] = jnp.zeros((8, 128), F32)
    req[KEY : KEY + 1, 0:20] = jnp.where(live, lists_in[1] * 64 + lists_in[0], -1).astype(F32)
    for i in range(3):
        req[HZ + i : HZ + i + 1, 0:20] = ((off[i] + (off[i] & 1)) >> 1).astype(F32) * livef
    req[LIVE : LIVE + 1, 0:20] = livef
    req[TILE : TILE + 1, 0:20] = livef * me.astype(F32)

    for c in bring[3:5]:
        c.wait()
    for s, first in ((0, 0), (1, 13)):
        def pack(f, _, s=s, first=first):
            for i in range(3):
                xp[s, f, i * 8 : i * 8 + 8, :] = ext[f, 3:11, 8 + first + i, :]
            return 0
        lax.fori_loop(0, 13, pack, 0)

    pl.semaphore_wait(barrier, len(partners) + 4 * (jnp.minimum(me, 1) + jnp.minimum(tiles - 1 - me, 1)))

    request = [
        remote(req, rq.at[me], s_rq.at[k], r_rq.at[me], d) for k, d in enumerate(others)
    ]
    for c in request:
        c.start()
    xcopy = []
    for s in range(2):
        xcopy.append(remote(xp.at[s, 0:DIRECT], xr.at[1 - s, 0:DIRECT], s_x.at[s], r_x.at[1 - s], xside[s]))
    for s in range(2):
        xcopy.append(remote(
            xp.at[s, DIRECT:13], xr.at[1 - s, DIRECT:13], s_x.at[2 + s], r_x.at[3 - s], xside[s]
        ))
    by_way = [remote(xp.at[s, DIRECT:13], relay, s_x.at[2 + s], r_relay, xside[1 - s]) for s in range(2)]
    onward = [
        remote(relay, xr.at[1 - s, DIRECT:13], s_relay, r_x.at[3 - s], {"gx": across}) for s in range(2)
    ]
    if relays:
        for s in range(2):
            @pl.when(far[s])
            def _(s=s):
                by_way[s].start()
    for s in range(2):
        xcopy[s].start()
    for s in range(2):
        @pl.when(jnp.logical_not(far[s]))
        def _(s=s):
            xcopy[2 + s].start()
    zrows = ((0, 11), (5, 0))
    zcopy = []
    for d in range(2):
        a, b = zrows[d]
        zcopy.append([
            remote(
                ext.at[f, 3 + a : 6 + a, 8:24], ext.at[f, b : b + 3, 8:24], s_z.at[2 * k + d], r_z.at[2 * k + d], zside[d]
            )
            for k, f in enumerate((slice(0, EARLY), slice(EARLY, 13)))
        ])

        @pl.when(has[d])
        def _(d=d):
            zcopy[d][0].start()


    row8, lane8 = iota((8, 128), 0), iota((8, 128), 1) >> 4
    bring[5].wait()

    def turn(g, _):
        rows = pl.ds(pl.multiple_of(g * 8, 8), 8)
        for c in range(32):
            v = stored[rows, c * 128 : c * 128 + 128]
            for k in (1, 2, 4):
                rb, lbit = (row8 & k) != 0, (lane8 & k) != 0
                a = pltpu.roll(pltpu.roll(v, 8 - k, 0), 16 * k, 1)
                b = pltpu.roll(pltpu.roll(v, k, 0), 128 - 16 * k, 1)
                v = jnp.where(rb == lbit, v, jnp.where(lbit, a, b))
            lb[g, c // 2, (c % 2) * 8 : (c % 2) * 8 + 8, :] = v
        return 0
    lax.fori_loop(0, 5, turn, 0)
    rq[me] = req[...]
    xs[...] = jnp.zeros(xs.shape, F32)

    for k in range(1, tiles):
        src = lax.rem(me + tiles - k, tiles)
        remote(req, rq.at[src], s_rq.at[k - 1], r_rq.at[src], others[k - 1]).wait_recv()

    if relays:
        for s in range(2):
            @pl.when(relaying[s])
            def _(s=s):
                by_way[s].wait_recv()
                onward[s].start()

    lists = [jnp.zeros((8, 128), F32), jnp.zeros((8, 128), F32)]
    for t in range(tiles):
        v = rq[t]
        lists[t // 4] = lists[t // 4] + (pltpu.roll(v, 32 * (t % 4), 1) if t % 4 else v)
    for h in range(2):
        prm[5 + h] = lists[h]
    base = me * 64
    for g in range(5):
        slot_of = base + g * 8 + (iota((128, 128), 0) >> 4)
        total = jnp.zeros((8, 128), F32)
        for h in range(2):
            match = jnp.where(lists[h][KEY : KEY + 1, :] == slot_of.astype(F32), 1.0, 0.0).astype(BF16)
            total = total + nt(lists[h].astype(BF16), match)
        prm[g] = total

    def choose(g, _):
        v = prm[g]
        hz, hx = v[HZ : HZ + 1, :], v[HX : HX + 1, :]
        layers = [jnp.zeros((16, 128), F32) for _ in range(5)]
        for p in range(16):
            part = lb[g, p]
            for a in range(5):
                layers[a] = layers[a] + jnp.where(hz == float(a - p), part, 0.0)
        at = iota((16, 128), 0).astype(F32) + hx
        lanes = pl.ds(pl.multiple_of(g * 128, 128), 128)
        for a in range(5):
            for b in range(AX):
                xs[a * AX + b : a * AX + b + 1, lanes] = jnp.sum(
                    jnp.where(at == float(b), layers[a], 0.0), axis=0, keepdims=True
                )
        return 0
    lax.fori_loop(0, 5, choose, 0)

    hi, lo = split(xs[...])
    both = jnp.concatenate([hi, lo], axis=0)
    where_to = []
    for g in range(5):
        v = prm[g]
        spot = v[HY : HY + 1, :] + 128.0 * v[TILE : TILE + 1, :] + (iota((1, 128), 1) & 15).astype(F32)
        where_to.append(jnp.where(v[LIVE : LIVE + 1, :] > 0.5, spot, -4096.0))
    where_to = jnp.concatenate(where_to, axis=1)
    tile_of = lax.rem(me + iota((8, 640), 0), tiles) * 128 + 64
    last = jnp.where(tile_of.astype(F32) == where_to, 1.0, 0.0).astype(BF16)
    blank = jnp.zeros((64, 640), BF16)
    tail = nt(last, jnp.concatenate([blank, hi, blank[0:16]], axis=0))
    tail = tail + nt(last, jnp.concatenate([blank, lo, blank[0:16]], axis=0))
    lane, at_last = iota((24, 128), 1), iota((24, 128), 0) == 23
    answer = []
    for k in range(tiles - 1, -1, -1):
        t = lax.rem(me + k, tiles)
        line = (iota((128, 640), 0) + t * 128).astype(F32)
        onto = jnp.where(line == where_to, 1.0, 0.0).astype(BF16)
        out = nt(both, onto)
        out = out[0:NODES] + out[NODES : 2 * NODES]
        upper = jnp.where(at_last, tail[k : k + 1, :], pltpu.roll(out[24:48], 64, 1))
        gr[t] = jnp.where(lane < 64, out[0:24], upper)
        if k:
            c = remote(gr.at[t], gx.at[me], s_gx.at[k - 1], r_gx.at[me], others[k - 1])
            c.start()
            answer.append(c)

    for d in range(2):
        @pl.when(has[d])
        def _(d=d):
            zcopy[d][1].start()

    inner, outer = slice(8, 24), slice(0, 8)
    def mirror(fields, rows):
        for d in range(2):
            @pl.when(jnp.logical_not(has[1 - d]))
            def _(d=d):
                def one(f, _):
                    for i in range(3):
                        if d:
                            ext[f, 2 - i, rows] = ext[f, 3 + i, rows]
                        else:
                            ext[f, 11 + i, rows] = ext[f, 10 - i, rows]
                    return 0
                lax.fori_loop(*fields, one, 0)

    def pack_y(rows, count):
        slot = iota((count, 128), 1) >> 3
        def one(f, _):
            v = jnp.zeros((count, 128), F32)
            for r in range(14):
                v = jnp.where(slot == r, pltpu.roll(ext[f, r, rows], r * 8 + 4, 1), v)
            pk[f, rows] = v
            return 0
        lax.fori_loop(0, 13, one, 0)

    def y_copies(rows, k):
        return [
            remote(pk.at[:, rows], yr.at[1, :, rows], s_y.at[k], r_y.at[k + 1], yside[0]),
            remote(pk.at[:, rows], yr.at[0, :, rows], s_y.at[k + 1], r_y.at[k], yside[1]),
        ]

    def unpack_y(rows, count):
        upper = (iota((count, 128), 1) & 7) >= 4
        def one(f, _):
            own = pk[f, rows]
            ext[f, LOW, rows] = jnp.where(upper, own, yr[0, f, rows])
            ext[f, HIGH, rows] = jnp.where(upper, yr[1, f, rows], own)
            return 0
        lax.fori_loop(0, 13, one, 0)

    def unpack_x(f):
        for z in range(8):
            ext[f, 3 + z, 0:3, :] = xr[1, f, pl.ds(z, 3, stride=8), :]
            ext[f, 3 + z, 5:8, :] = xr[0, f, pl.ds(z, 3, stride=8), :]

    bz, bx, by = [
        jnp.max(jnp.where(live, o & 1, 0).astype(F32), axis=1, keepdims=True) for o in off
    ]
    node, cell = iota((128, 128), 0), iota((128, 128), 1).astype(F32)
    wy = jnp.maximum(0.0, 1.0 - jnp.abs(cell - (2.0 * node.astype(F32) - by)) * 0.5)
    wy = jnp.where(node < 64, wy, 0.0).astype(BF16)
    w64 = jnp.maximum(0.0, 1.0 - jnp.abs(iota((1, 128), 1).astype(F32) - (128.0 - by)) * 0.5)
    ci, ki = iota((128, NODES), 0), iota((128, NODES), 1)
    az = (ki * 57) >> 9
    ax = ki - AX * az
    wz = jnp.maximum(0.0, 1.0 - jnp.abs((ci >> 4).astype(F32) - (2.0 * az.astype(F32) - bz)) * 0.5)
    wx = jnp.maximum(0.0, 1.0 - jnp.abs((ci & 15).astype(F32) - (2.0 * ax.astype(F32) - bx)) * 0.5)
    wzx32 = wz * wx
    wzx = wzx32.astype(BF16)

    grid = gr[me]
    for k in range(1, tiles):
        src = lax.rem(me + tiles - k, tiles)
        remote(gr.at[src], gx.at[src], s_gx.at[k - 1], r_gx.at[src], others[k - 1]).wait_recv()
        grid = grid + gx[src]
    turned = pltpu.roll(grid, 64, 1)
    column = jnp.sum(wzx32 * turned[23:24, 0:NODES], axis=1, keepdims=True)
    hi, lo = split(jnp.concatenate([grid, turned], axis=0))
    fine = jnp.dot(jnp.concatenate([hi, lo], axis=0), wy, preferred_element_type=F32)
    fine = fine[0:NODES] + fine[NODES : 2 * NODES]
    hi, lo = split(fine)
    heat = jnp.dot(wzx, hi, preferred_element_type=F32) + jnp.dot(wzx, lo, preferred_element_type=F32)
    heat = heat + column * w64
    heat = heat.reshape(8, 16, 128)
    heat_out[...] = heat
    for z in range(8):
        ext[HEAT, 3 + z, 8:24, :] = heat[z]
    for s, first in ((0, 0), (1, 13)):
        for i in range(3):
            xp[s, HEAT, i * 8 : i * 8 + 8, :] = heat[:, first + i, :]
    xheat = [
        remote(xp.at[0, HEAT], xr.at[1, HEAT], s_xt.at[0], r_xt.at[1], xside[0]),
        remote(xp.at[1, HEAT], xr.at[0, HEAT], s_xt.at[1], r_xt.at[0], xside[1]),
    ]
    for c in xheat:
        c.start()
    zheat = []
    for d in range(2):
        a, b = zrows[d]
        zheat.append(remote(
            ext.at[HEAT, 3 + a : 6 + a, 8:24], ext.at[HEAT, b : b + 3, 8:24], s_zt.at[d], r_zt.at[d], zside[d]
        ))

        @pl.when(has[d])
        def _(d=d):
            zheat[d].start()

    for z in range(8):
        v = pltpu.roll(heat[z], (z + 3) * 8 + 4, 1)
        strips = v if z == 0 else jnp.where((iota((16, 128), 1) >> 3) == z + 3, v, strips)
    hk[...] = strips
    yheat, xyheat, xzheat, yzheat = [], [], [], []
    for t in range(2):
        yheat.append(remote(hk, hy.at[1 - t], s_hy.at[t], r_hy.at[1 - t], yside[t]))
        for s in range(2):
            n = 2 * (1 - t) + 1 - s
            xyheat.append(remote(
                hk.at[8 * s : 8 * s + 8], hxy.at[n], s_hxy.at[2 * t + s], r_hxy.at[n], xy[t][s]
            ))
    for c in (*xyheat, *yheat):
        c.start()
    for d in range(2):
        for s in range(2):
            n = 2 * d + 1 - s
            xzheat.append(remote(
                ext.at[HEAT, (3, 10)[d], 8 * s + 8 : 8 * s + 16], hxz.at[n], s_hxz.at[2 * d + s], r_hxz.at[n], xz[d][s]
            ))
        for t in range(2):
            n = 2 * d + 1 - t
            yzheat.append(remote(hk, hyz.at[n], s_hyz.at[2 * d + t], r_hyz.at[n], yz[t][d]))

        @pl.when(has[d])
        def _(d=d):
            for k in (2 * d, 2 * d + 1):
                xzheat[k].start()
                yzheat[k].start()

    for c in xcopy:
        c.wait_recv()

    order = ((2, 1), (0, 1))
    shown = ((0, 1), (7, 6))
    dcopy = []
    for d in range(2):
        for s in range(2):
            near, far = order[s]
            z1, z2 = shown[d]
            for k, (i, z) in enumerate(((near, z1), (near, z2), (far, z1))):
                for f in range(13):
                    dp[2 * d + s, k, f : f + 1, :] = xr[s, f, i * 8 + z : i * 8 + z + 1, :]
            dcopy.append(remote(
                dp.at[2 * d + s], dr.at[2 * d + s], s_d.at[2 * d + s], r_d.at[2 * d + s], zside[d]
            ))

        @pl.when(has[d])
        def _(d=d):
            for s in range(2):
                dcopy[2 * d + s].start()

    def unpack_all(f, _):
        unpack_x(f)
        return 0
    lax.fori_loop(0, 13, unpack_all, 0)

    for d in range(2):
        @pl.when(has[1 - d])
        def _(d=d):
            for c in zcopy[d]:
                c.wait_recv()
    mirror((0, 13), inner)
    pack_y(inner, 16)
    yinner = y_copies(inner, 0)
    for c in yinner:
        c.start()

    for d in range(2):
        @pl.when(has[1 - d])
        def _(d=d):
            for s in range(2):
                dcopy[2 * d + s].wait_recv()
            e1, e2 = ((11, 12), (2, 1))[d]
            for s in range(2):
                x1, x2 = ((7, 6), (0, 1))[s]
                for k, (e, x) in enumerate(((e1, x1), (e2, x1), (e1, x2))):
                    for f in range(13):
                        ext[f, e, x : x + 1, :] = dr[2 * d + s, k, f : f + 1, :]
    mirror((0, 13), outer)

    pack_y(outer, 8)
    youter = y_copies(outer, 2)
    for c in youter:
        c.start()

    for c in (*xheat, *yheat):
        c.wait_recv()
    for c in xyheat:
        c.wait_recv()
    unpack_x(HEAT)
    lane16, slot16, row8 = iota((16, 128), 1), iota((16, 128), 1) >> 3, iota((8, 128), 0)
    theirs = ((lane16 & 7) < 4, (lane16 & 7) >= 4)
    for p in range(2):
        ext[HEAT, LOW + p, inner] = jnp.where(theirs[p], hy[p], strips)
        ext[HEAT, LOW + p, outer] = jnp.where(row8 < 4, hxy[2 * p + 1], hxy[2 * p])
    mirror((HEAT, HEAT + 1), slice(0, 24))
    for d in range(2):
        new = (11, 2)[d]

        @pl.when(has[1 - d])
        def _(d=d, new=new):
            zheat[d].wait_recv()
            for k in (2 * d, 2 * d + 1):
                xzheat[k].wait_recv()
                yzheat[k].wait_recv()
            ext[HEAT, new, outer] = jnp.where(row8 < 4, hxz[2 * d + 1], hxz[2 * d])
            for p in range(2):
                ext[HEAT, LOW + p, inner] = jnp.where(
                    theirs[p] & (slot16 == new), pltpu.roll(hyz[2 * d + p], 64, 1), ext[HEAT, LOW + p, inner]
                )

        @pl.when(jnp.logical_not(has[1 - d]))
        def _(d=d, new=new):
            for p in range(2):
                v = ext[HEAT, LOW + p, inner]
                ext[HEAT, LOW + p, inner] = jnp.where(
                    theirs[p] & (slot16 == new), pltpu.roll(v, (8, 120)[d], 1), v
                )

    for c in youter:
        c.wait_recv()
    unpack_y(outer, 8)
    for c in yinner:
        c.wait_recv()
    unpack_y(inner, 16)

    def step(src, dst, first, last):
        cells = slice(0, 24)

        def sums(r, _):
            s = src[0, r, cells] * src[0, r, cells]
            for f in range(1, 12):
                s = s + src[f, r, cells] * src[f, r, cells]
            u = src[SOL, r, cells]
            squares[r] = 0.1 * s - 0.04
            bend[r, cells] = u - 0.5 * s
            drives[r] = 6.0 * (1.0 - ext[HEAT, r, cells] - 0.5 * u)
            return 0
        lax.fori_loop(0, 16, sums, 0, unroll=4)
        final = dst is None
        groups = [(a, b, range(first, last)) for a, b in GROUPS[0:2]]
        if not final:
            groups.append((*GROUPS[2], range(first + 1, last - 1)))
        strips = groups[0 : 3 if first == 1 else 2]

        def fields(f, _):
            now = src.at[f]
            for a, b, rows in groups:
                edge = edges(now[LOW, a:b, :], now[HIGH, a:b, :])
                for r in rows:
                    c, around = main_neighbours(now, r, a, edge)
                    v = grown(c, around, squares[r, a:b], drives[r, a:b])
                    if final:
                        grains_out[f, r - 3, a - 8 : b - 8, :] = v
                    else:
                        dst[f, r, a:b, :] = v
            if not final:
                for a, b, _ in strips:
                    for r in (LOW, HIGH):
                        c, around = strip_neighbours(now, r, a)
                        dst[f, r, a:b, :] = grown(c, around, squares[r, a:b], drives[r, a:b])
            return 0
        lax.fori_loop(0, 12, fields, 0)
        for a, b, rows in groups:
            edge = edges(bend[LOW, a:b, :], bend[HIGH, a:b, :])
            for r in rows:
                c, around = main_neighbours(bend, r, a, edge)
                v = src[SOL, r, a:b, :] + 0.15 * (around - 6.0 * c)
                if final:
                    solute_out[r - 3, a - 8 : b - 8, :] = v
                else:
                    dst[SOL, r, a:b, :] = v
        if not final:
            for a, b, _ in strips:
                for r in (LOW, HIGH):
                    c, around = strip_neighbours(bend, r, a)
                    dst[SOL, r, a:b, :] = src[SOL, r, a:b, :] + 0.15 * (around - 6.0 * c)

    step(ext, alt, 1, 13)
    for d in range(2):
        @pl.when(has[d])
        def _(d=d):
            for c in zcopy[d]:
                c.wait_send()

    step(alt, ext, 2, 12)
    step(ext, None, 3, 11)

    for c in [*request, *xcopy, *answer, *xheat, *yinner, *youter, *yheat, *xyheat]:
        c.wait_send()
    for d in range(2):
        @pl.when(has[d])
        def _(d=d):
            for k in (2 * d, 2 * d + 1):
                for c in (dcopy[k], xzheat[k], yzheat[k]):
                    c.wait_send()
            zheat[d].wait_send()
    if relays:
        @pl.when(relaying[0] | relaying[1])
        def _():
            onward[0].wait_send()


def body(grains, solute, thermal, block_slot, block_owner, block_offset):
    tiles = lax.axis_size("gz")
    vmem = pl.BlockSpec(memory_space=pltpu.VMEM)
    dma = pltpu.SemaphoreType.DMA
    import functools

    return pl.pallas_call(
        functools.partial(kernel, tiles),
        out_shape=(
            jax.ShapeDtypeStruct(grains.shape, F32),
            jax.ShapeDtypeStruct(solute.shape, F32),
            jax.ShapeDtypeStruct(solute.shape, F32),
        ),
        in_specs=[pl.BlockSpec(memory_space=pltpu.HBM)] * 6,
        out_specs=(vmem,) * 3,
        scratch_shapes=[
            pltpu.VMEM((NF, 16, 32, 128), F32),
            pltpu.VMEM((13, 16, 32, 128), F32),
            pltpu.VMEM((16, 32, 128), F32),
            pltpu.VMEM((16, 24, 128), F32),
            pltpu.VMEM((16, 24, 128), F32),
            pltpu.VMEM((2, NF, 24, 128), F32),
            pltpu.VMEM((2, NF, 24, 128), F32),
            pltpu.VMEM((13 - DIRECT, 24, 128), F32),
            pltpu.VMEM((4, 3, 16, 128), F32),
            pltpu.VMEM((4, 3, 16, 128), F32),
            pltpu.VMEM((13, 24, 128), F32),
            pltpu.VMEM((2, 13, 24, 128), F32),
            pltpu.VMEM((16, 128), F32),
            pltpu.VMEM((2, 16, 128), F32),
            pltpu.VMEM((4, 8, 128), F32),
            pltpu.VMEM((4, 8, 128), F32),
            pltpu.VMEM((4, 16, 128), F32),
            pltpu.VMEM((40, 4096), F32),
            pltpu.VMEM((5, 1, 20), jnp.int32),
            pltpu.VMEM((8, 128), F32),
            pltpu.VMEM((tiles, 8, 128), F32),
            pltpu.VMEM((5, 16, 16, 128), F32),
            pltpu.VMEM((7, 8, 128), F32),
            pltpu.VMEM((NODES, 640), F32),
            pltpu.VMEM((tiles, 24, 128), F32),
            pltpu.VMEM((tiles, 24, 128), F32),
            dma((6,)), dma((tiles,)), dma((tiles,)), dma((tiles,)), dma((tiles,)),
            dma((4,)), dma((4,)), dma((4,)), dma((4,)),
            dma((2,)), dma((2,)), dma((2,)), dma((2,)),
            dma((4,)), dma((4,)), dma((4,)), dma((4,)),
            dma, dma, dma((2,)), dma((2,)), dma((4,)), dma((4,)),
            dma((4,)), dma((4,)), dma((4,)), dma((4,)),
        ],
        compiler_params=pltpu.CompilerParams(
            collective_id=0, has_side_effects=True, vmem_limit_bytes=50331648
        ),
    )(*(
        pltpu.with_memory_space_constraint(a, pltpu.HBM)
        for a in (
            grains,
            solute,
            thermal.reshape(thermal.shape[3], thermal.shape[4]),
            block_slot.reshape(1, -1),
            block_owner.reshape(1, -1),
            block_offset.reshape(3, 1, -1),
        )
    ))


def solution(mesh):
    in_specs = (
        P(None, "gz", "gx", "gy"),
        P("gz", "gx", "gy"),
        P("gz", "gx", "gy", None, None),
        P("gz", "gx", "gy", None),
        P("gz", "gx", "gy", None),
        P("gz", "gx", "gy", None, None),
    )
    out_specs = (P(None, "gz", "gx", "gy"), P("gz", "gx", "gy"), P("gz", "gx", "gy"))
    return jax.shard_map(body, mesh=mesh, in_specs=in_specs, out_specs=out_specs, check_vma=False)
```

```python
import jax
import jax.numpy as jnp
from jax import lax
from jax.experimental import pallas as pl
from jax.experimental.pallas import tpu as pltpu
from jax.sharding import PartitionSpec as P

F32 = jnp.float32
BF16 = jnp.bfloat16
MESH = pl.DeviceIdType.MESH
NF = 14
SOL = 12
HEAT = 13
DIRECT = 4
EARLY = 7
KEY, HZ, HX, HY, LIVE, TILE = range(6)
AX = 9
NODES = 48
LOW, HIGH = 14, 15


def iota(shape, axis):
    return lax.broadcasted_iota(jnp.int32, shape, axis)


def split(x):
    high = x.astype(BF16)
    return high, (x - high.astype(F32)).astype(BF16)


def nt(a, b):
    return lax.dot_general(a, b, (((1,), (1,)), ((), ())), preferred_element_type=F32)


GROUPS = ((8, 16), (16, 24), (0, 8))


def edges(low, high):
    return jnp.where((iota(low.shape, 1) & 7) == 3, low, pltpu.roll(high, 126, 1))


def along_x(ref, r, a):
    sub = iota((8, 128), 0)
    if a == 0:
        before = jnp.where(sub == 0, ref[r, 23:24, :], pltpu.roll(ref[r, 0:8, :], 1, 0))
        return before + ref[r, 1:9, :]
    after = ref[r, a + 1 : a + 9, :]
    if a == 16:
        after = jnp.where(sub == 7, ref[r, 0:1, :], after)
    return ref[r, a - 1 : a + 7, :] + after


def main_neighbours(ref, r, a, edge):
    lane = iota((8, 128), 1)
    c = ref[r, a : a + 8, :]
    beyond = pltpu.roll(edge, (125 - r * 8) % 128, 1)
    left = jnp.where(lane == 0, beyond, pltpu.roll(c, 1, 1))
    right = jnp.where(lane == 127, beyond, pltpu.roll(c, 127, 1))
    return c, (ref[r - 1, a : a + 8, :] + ref[r + 1, a : a + 8, :]) + along_x(ref, r, a) + (left + right)


def strip_neighbours(ref, r, a):
    c = ref[r, a : a + 8, :]
    z = pltpu.roll(c, 8, 1) + pltpu.roll(c, 120, 1)
    y = pltpu.roll(c, 1, 1) + pltpu.roll(c, 127, 1)
    return c, z + y + along_x(ref, r, a)


def grown(c, around, s, drive):
    cc = c * c
    w = c - cc
    return w * ((0.4 * c - 0.2) + w * drive) + c * (0.1 * cc - s) + 0.16 * around


def kernel(
    tiles,
    grains, solute, thermal, slots, owners, offsets,
    grains_out, solute_out, heat_out,
    ext, alt, bend, squares, drives,
    xp, xr, relay, dp, dr, pk, yr,
    hk, hy, hxz, hxy, hyz,
    stored, lists_in, req, rq, lb, prm, xs, gr, gx,
    loads, s_rq, r_rq, s_gx, r_gx, s_z, r_z, s_x, r_x, s_zt, r_zt, s_xt, r_xt, s_d, r_d, s_y, r_y,
    s_relay, r_relay, s_hy, r_hy, s_hxz, r_hxz, s_hxy, r_hxy, s_hyz, r_hyz,
):
    me = lax.axis_index("gz")
    ix, iy = lax.axis_index("gx"), lax.axis_index("gy")
    nx, ny = lax.axis_size("gx"), lax.axis_size("gy")
    xside = ({"gx": lax.rem(ix + nx - 1, nx)}, {"gx": lax.rem(ix + 1, nx)})
    yside = ({"gy": lax.rem(iy + ny - 1, ny)}, {"gy": lax.rem(iy + 1, ny)})
    others = [{"gz": lax.rem(me + k, tiles)} for k in range(1, tiles)]
    has_low, has_high = me > 0, me < tiles - 1
    relays = nx == 8
    ax4 = lax.rem(ix, 4)
    far = (ax4 == 0, ax4 == 3) if relays else (ix < 0, ix < 0)
    relaying = (ax4 == 1, ax4 == 2)
    across = 6 + 2 * lax.rem(ix, 2) - ix
    zside = ({"gz": jnp.maximum(me - 1, 0)}, {"gz": jnp.minimum(me + 1, tiles - 1)})
    has = (has_low, has_high)

    bring = [
        pltpu.make_async_copy(slots, lists_in.at[0], loads.at[0]),
        pltpu.make_async_copy(owners, lists_in.at[1], loads.at[1]),
        pltpu.make_async_copy(offsets, lists_in.at[2:5], loads.at[2]),
        pltpu.make_async_copy(grains, ext.at[0:12, 3:11, 8:24], loads.at[3]),
        pltpu.make_async_copy(solute, ext.at[SOL, 3:11, 8:24], loads.at[4]),
        pltpu.make_async_copy(thermal, stored, loads.at[5]),
    ]
    for c in bring:
        c.start()

    barrier = pltpu.get_barrier_semaphore()
    xy = [[{**xside[s], **yside[t]} for s in range(2)] for t in range(2)]
    xz = [[{**xside[s], **zside[d]} for s in range(2)] for d in range(2)]
    yz = [[{**yside[t], **zside[d]} for d in range(2)] for t in range(2)]
    partners = [*xside, *yside, *others, *xy[0], *xy[1]]
    if relays:
        partners.append({"gx": across})
    for d in partners:
        pl.semaphore_signal(barrier, inc=1, device_id=d, device_id_type=MESH)
    for d in range(2):
        @pl.when(has[d])
        def _(d=d):
            for p in (*xz[d], yz[0][d], yz[1][d]):
                pl.semaphore_signal(barrier, inc=1, device_id=p, device_id_type=MESH)

    def remote(src, dst, ss, rs, d):
        return pltpu.make_async_remote_copy(
            src_ref=src, dst_ref=dst, send_sem=ss, recv_sem=rs, device_id=d, device_id_type=MESH
        )

    for c in bring[0:3]:
        c.wait()
    live = lists_in[1] >= 0
    livef = live.astype(F32)
    off = [lists_in[2 + i] for i in range(3)]
    req[...] = jnp.zeros((8, 128), F32)
    req[KEY : KEY + 1, 0:20] = jnp.where(live, lists_in[1] * 64 + lists_in[0], -1).astype(F32)
    for i in range(3):
        req[HZ + i : HZ + i + 1, 0:20] = ((off[i] + (off[i] & 1)) >> 1).astype(F32) * livef
    req[LIVE : LIVE + 1, 0:20] = livef
    req[TILE : TILE + 1, 0:20] = livef * me.astype(F32)

    for c in bring[3:5]:
        c.wait()
    for s, first in ((0, 0), (1, 13)):
        def pack(f, _, s=s, first=first):
            for i in range(3):
                xp[s, f, i * 8 : i * 8 + 8, :] = ext[f, 3:11, 8 + first + i, :]
            return 0
        lax.fori_loop(0, 13, pack, 0)

    pl.semaphore_wait(barrier, len(partners) + 4 * (jnp.minimum(me, 1) + jnp.minimum(tiles - 1 - me, 1)))

    request = [
        remote(req, rq.at[me], s_rq.at[k], r_rq.at[me], d) for k, d in enumerate(others)
    ]
    for c in request:
        c.start()
    xcopy = []
    for s in range(2):
        xcopy.append(remote(xp.at[s, 0:DIRECT], xr.at[1 - s, 0:DIRECT], s_x.at[s], r_x.at[1 - s], xside[s]))
    for s in range(2):
        xcopy.append(remote(
            xp.at[s, DIRECT:13], xr.at[1 - s, DIRECT:13], s_x.at[2 + s], r_x.at[3 - s], xside[s]
        ))
    by_way = [remote(xp.at[s, DIRECT:13], relay, s_x.at[2 + s], r_relay, xside[1 - s]) for s in range(2)]
    onward = [
        remote(relay, xr.at[1 - s, DIRECT:13], s_relay, r_x.at[3 - s], {"gx": across}) for s in range(2)
    ]
    if relays:
        for s in range(2):
            @pl.when(far[s])
            def _(s=s):
                by_way[s].start()
    for s in range(2):
        xcopy[s].start()
    for s in range(2):
        @pl.when(jnp.logical_not(far[s]))
        def _(s=s):
            xcopy[2 + s].start()
    zrows = ((0, 11), (5, 0))
    zcopy = []
    for d in range(2):
        a, b = zrows[d]
        zcopy.append([
            remote(
                ext.at[f, 3 + a : 6 + a, 8:24], ext.at[f, b : b + 3, 8:24], s_z.at[2 * k + d], r_z.at[2 * k + d], zside[d]
            )
            for k, f in enumerate((slice(0, EARLY), slice(EARLY, 13)))
        ])

        @pl.when(has[d])
        def _(d=d):
            zcopy[d][0].start()


    row8, lane8 = iota((8, 128), 0), iota((8, 128), 1) >> 4
    bring[5].wait()

    def turn(g, _):
        rows = pl.ds(pl.multiple_of(g * 8, 8), 8)
        for c in range(32):
            v = stored[rows, c * 128 : c * 128 + 128]
            for k in (1, 2, 4):
                rb, lbit = (row8 & k) != 0, (lane8 & k) != 0
                a = pltpu.roll(pltpu.roll(v, 8 - k, 0), 16 * k, 1)
                b = pltpu.roll(pltpu.roll(v, k, 0), 128 - 16 * k, 1)
                v = jnp.where(rb == lbit, v, jnp.where(lbit, a, b))
            lb[g, c // 2, (c % 2) * 8 : (c % 2) * 8 + 8, :] = v
        return 0
    lax.fori_loop(0, 5, turn, 0)
    rq[me] = req[...]
    xs[...] = jnp.zeros(xs.shape, F32)

    for k in range(1, tiles):
        src = lax.rem(me + tiles - k, tiles)
        remote(req, rq.at[src], s_rq.at[k - 1], r_rq.at[src], others[k - 1]).wait_recv()

    if relays:
        for s in range(2):
            @pl.when(relaying[s])
            def _(s=s):
                by_way[s].wait_recv()
                onward[s].start()

    lists = [jnp.zeros((8, 128), F32), jnp.zeros((8, 128), F32)]
    for t in range(tiles):
        v = rq[t]
        lists[t // 4] = lists[t // 4] + (pltpu.roll(v, 32 * (t % 4), 1) if t % 4 else v)
    for h in range(2):
        prm[5 + h] = lists[h]
    base = me * 64
    for g in range(5):
        slot_of = base + g * 8 + (iota((128, 128), 0) >> 4)
        total = jnp.zeros((8, 128), F32)
        for h in range(2):
            match = jnp.where(lists[h][KEY : KEY + 1, :] == slot_of.astype(F32), 1.0, 0.0).astype(BF16)
            total = total + nt(lists[h].astype(BF16), match)
        prm[g] = total

    def choose(g, _):
        v = prm[g]
        hz, hx = v[HZ : HZ + 1, :], v[HX : HX + 1, :]
        layers = [jnp.zeros((16, 128), F32) for _ in range(5)]
        for p in range(16):
            part = lb[g, p]
            for a in range(5):
                layers[a] = layers[a] + jnp.where(hz == float(a - p), part, 0.0)
        at = iota((16, 128), 0).astype(F32) + hx
        lanes = pl.ds(pl.multiple_of(g * 128, 128), 128)
        for a in range(5):
            for b in range(AX):
                xs[a * AX + b : a * AX + b + 1, lanes] = jnp.sum(
                    jnp.where(at == float(b), layers[a], 0.0), axis=0, keepdims=True
                )
        return 0
    lax.fori_loop(0, 5, choose, 0)

    hi, lo = split(xs[...])
    both = jnp.concatenate([hi, lo], axis=0)
    where_to = []
    for g in range(5):
        v = prm[g]
        spot = v[HY : HY + 1, :] + 128.0 * v[TILE : TILE + 1, :] + (iota((1, 128), 1) & 15).astype(F32)
        where_to.append(jnp.where(v[LIVE : LIVE + 1, :] > 0.5, spot, -4096.0))
    where_to = jnp.concatenate(where_to, axis=1)
    tile_of = lax.rem(me + iota((8, 640), 0), tiles) * 128 + 64
    last = jnp.where(tile_of.astype(F32) == where_to, 1.0, 0.0).astype(BF16)
    blank = jnp.zeros((64, 640), BF16)
    tail = nt(last, jnp.concatenate([blank, hi, blank[0:16]], axis=0))
    tail = tail + nt(last, jnp.concatenate([blank, lo, blank[0:16]], axis=0))
    lane, at_last = iota((24, 128), 1), iota((24, 128), 0) == 23
    answer = []
    for k in range(tiles - 1, -1, -1):
        t = lax.rem(me + k, tiles)
        line = (iota((128, 640), 0) + t * 128).astype(F32)
        onto = jnp.where(line == where_to, 1.0, 0.0).astype(BF16)
        out = nt(both, onto)
        out = out[0:NODES] + out[NODES : 2 * NODES]
        upper = jnp.where(at_last, tail[k : k + 1, :], pltpu.roll(out[24:48], 64, 1))
        gr[t] = jnp.where(lane < 64, out[0:24], upper)
        if k:
            c = remote(gr.at[t], gx.at[me], s_gx.at[k - 1], r_gx.at[me], others[k - 1])
            c.start()
            answer.append(c)

    for d in range(2):
        @pl.when(has[d])
        def _(d=d):
            zcopy[d][1].start()

    inner, outer = slice(8, 24), slice(0, 8)
    def mirror(fields, rows):
        for d in range(2):
            @pl.when(jnp.logical_not(has[1 - d]))
            def _(d=d):
                def one(f, _):
                    for i in range(3):
                        if d:
                            ext[f, 2 - i, rows] = ext[f, 3 + i, rows]
                        else:
                            ext[f, 11 + i, rows] = ext[f, 10 - i, rows]
                    return 0
                lax.fori_loop(*fields, one, 0)

    def pack_y(rows, count):
        slot = iota((count, 128), 1) >> 3
        def one(f, _):
            v = jnp.zeros((count, 128), F32)
            for r in range(14):
                v = jnp.where(slot == r, pltpu.roll(ext[f, r, rows], r * 8 + 4, 1), v)
            pk[f, rows] = v
            return 0
        lax.fori_loop(0, 13, one, 0)

    def y_copies(rows, k):
        return [
            remote(pk.at[:, rows], yr.at[1, :, rows], s_y.at[k], r_y.at[k + 1], yside[0]),
            remote(pk.at[:, rows], yr.at[0, :, rows], s_y.at[k + 1], r_y.at[k], yside[1]),
        ]

    def unpack_y(rows, count):
        upper = (iota((count, 128), 1) & 7) >= 4
        def one(f, _):
            own = pk[f, rows]
            ext[f, LOW, rows] = jnp.where(upper, own, yr[0, f, rows])
            ext[f, HIGH, rows] = jnp.where(upper, yr[1, f, rows], own)
            return 0
        lax.fori_loop(0, 13, one, 0)

    def unpack_x(f):
        for z in range(8):
            ext[f, 3 + z, 0:3, :] = xr[1, f, pl.ds(z, 3, stride=8), :]
            ext[f, 3 + z, 5:8, :] = xr[0, f, pl.ds(z, 3, stride=8), :]

    bz, bx, by = [
        jnp.max(jnp.where(live, o & 1, 0).astype(F32), axis=1, keepdims=True) for o in off
    ]
    node, cell = iota((128, 128), 0), iota((128, 128), 1).astype(F32)
    wy = jnp.maximum(0.0, 1.0 - jnp.abs(cell - (2.0 * node.astype(F32) - by)) * 0.5)
    wy = jnp.where(node < 64, wy, 0.0).astype(BF16)
    w64 = jnp.maximum(0.0, 1.0 - jnp.abs(iota((1, 128), 1).astype(F32) - (128.0 - by)) * 0.5)
    ci, ki = iota((128, NODES), 0), iota((128, NODES), 1)
    az = (ki * 57) >> 9
    ax = ki - AX * az
    wz = jnp.maximum(0.0, 1.0 - jnp.abs((ci >> 4).astype(F32) - (2.0 * az.astype(F32) - bz)) * 0.5)
    wx = jnp.maximum(0.0, 1.0 - jnp.abs((ci & 15).astype(F32) - (2.0 * ax.astype(F32) - bx)) * 0.5)
    wzx32 = wz * wx
    wzx = wzx32.astype(BF16)

    grid = gr[me]
    for k in range(1, tiles):
        src = lax.rem(me + tiles - k, tiles)
        remote(gr.at[src], gx.at[src], s_gx.at[k - 1], r_gx.at[src], others[k - 1]).wait_recv()
        grid = grid + gx[src]
    turned = pltpu.roll(grid, 64, 1)
    column = jnp.sum(wzx32 * turned[23:24, 0:NODES], axis=1, keepdims=True)
    hi, lo = split(jnp.concatenate([grid, turned], axis=0))
    fine = jnp.dot(jnp.concatenate([hi, lo], axis=0), wy, preferred_element_type=F32)
    fine = fine[0:NODES] + fine[NODES : 2 * NODES]
    hi, lo = split(fine)
    heat = jnp.dot(wzx, hi, preferred_element_type=F32) + jnp.dot(wzx, lo, preferred_element_type=F32)
    heat = heat + column * w64
    heat = heat.reshape(8, 16, 128)
    heat_out[...] = heat
    for z in range(8):
        ext[HEAT, 3 + z, 8:24, :] = heat[z]
    for s, first in ((0, 0), (1, 13)):
        for i in range(3):
            xp[s, HEAT, i * 8 : i * 8 + 8, :] = heat[:, first + i, :]
    xheat = [
        remote(xp.at[0, HEAT], xr.at[1, HEAT], s_xt.at[0], r_xt.at[1], xside[0]),
        remote(xp.at[1, HEAT], xr.at[0, HEAT], s_xt.at[1], r_xt.at[0], xside[1]),
    ]
    for c in xheat:
        c.start()
    zheat = []
    for d in range(2):
        a, b = zrows[d]
        zheat.append(remote(
            ext.at[HEAT, 3 + a : 6 + a, 8:24], ext.at[HEAT, b : b + 3, 8:24], s_zt.at[d], r_zt.at[d], zside[d]
        ))

        @pl.when(has[d])
        def _(d=d):
            zheat[d].start()

    for z in range(8):
        v = pltpu.roll(heat[z], (z + 3) * 8 + 4, 1)
        strips = v if z == 0 else jnp.where((iota((16, 128), 1) >> 3) == z + 3, v, strips)
    hk[...] = strips
    yheat, xyheat, xzheat, yzheat = [], [], [], []
    for t in range(2):
        yheat.append(remote(hk, hy.at[1 - t], s_hy.at[t], r_hy.at[1 - t], yside[t]))
        for s in range(2):
            n = 2 * (1 - t) + 1 - s
            xyheat.append(remote(
                hk.at[8 * s : 8 * s + 8], hxy.at[n], s_hxy.at[2 * t + s], r_hxy.at[n], xy[t][s]
            ))
    for c in (*xyheat, *yheat):
        c.start()
    for d in range(2):
        for s in range(2):
            n = 2 * d + 1 - s
            xzheat.append(remote(
                ext.at[HEAT, (3, 10)[d], 8 * s + 8 : 8 * s + 16], hxz.at[n], s_hxz.at[2 * d + s], r_hxz.at[n], xz[d][s]
            ))
        for t in range(2):
            n = 2 * d + 1 - t
            yzheat.append(remote(hk, hyz.at[n], s_hyz.at[2 * d + t], r_hyz.at[n], yz[t][d]))

        @pl.when(has[d])
        def _(d=d):
            for k in (2 * d, 2 * d + 1):
                xzheat[k].start()
                yzheat[k].start()

    for c in xcopy:
        c.wait_recv()

    order = ((2, 1), (0, 1))
    shown = ((0, 1), (7, 6))
    dcopy = []
    for d in range(2):
        for s in range(2):
            near, far = order[s]
            z1, z2 = shown[d]
            for k, (i, z) in enumerate(((near, z1), (near, z2), (far, z1))):
                for f in range(13):
                    dp[2 * d + s, k, f : f + 1, :] = xr[s, f, i * 8 + z : i * 8 + z + 1, :]
            dcopy.append(remote(
                dp.at[2 * d + s], dr.at[2 * d + s], s_d.at[2 * d + s], r_d.at[2 * d + s], zside[d]
            ))

        @pl.when(has[d])
        def _(d=d):
            for s in range(2):
                dcopy[2 * d + s].start()

    def unpack_all(f, _):
        unpack_x(f)
        return 0
    lax.fori_loop(0, 13, unpack_all, 0)

    for d in range(2):
        @pl.when(has[1 - d])
        def _(d=d):
            for c in zcopy[d]:
                c.wait_recv()
    mirror((0, 13), inner)
    pack_y(inner, 16)
    yinner = y_copies(inner, 0)
    for c in yinner:
        c.start()

    for d in range(2):
        @pl.when(has[1 - d])
        def _(d=d):
            for s in range(2):
                dcopy[2 * d + s].wait_recv()
            e1, e2 = ((11, 12), (2, 1))[d]
            for s in range(2):
                x1, x2 = ((7, 6), (0, 1))[s]
                for k, (e, x) in enumerate(((e1, x1), (e2, x1), (e1, x2))):
                    for f in range(13):
                        ext[f, e, x : x + 1, :] = dr[2 * d + s, k, f : f + 1, :]
    mirror((0, 13), outer)

    pack_y(outer, 8)
    youter = y_copies(outer, 2)
    for c in youter:
        c.start()

    for c in yinner:
        c.wait_recv()
    unpack_y(inner, 16)

    def sums_of(src, r):
        cells = slice(0, 24)
        s = src[0, r, cells] * src[0, r, cells]
        for f in range(1, 12):
            s = s + src[f, r, cells] * src[f, r, cells]
        squares[r] = 0.1 * s - 0.04
        bend[r, cells] = src[SOL, r, cells] - 0.5 * s

    def early_sums(r, _):
        sums_of(ext, r)
        return 0
    lax.fori_loop(0, 14, early_sums, 0, unroll=2)
    for r in range(3, 11):
        drives[r, inner] = 6.0 * (1.0 - ext[HEAT, r, inner] - 0.5 * ext[SOL, r, inner])

    def early_fields(f, _):
        now = ext.at[f]
        for a, b in GROUPS[0:2]:
            edge = edges(now[LOW, a:b, :], now[HIGH, a:b, :])
            for r in range(3, 11):
                c, around = main_neighbours(now, r, a, edge)
                alt[f, r, a:b, :] = grown(c, around, squares[r, a:b], drives[r, a:b])
        return 0
    lax.fori_loop(0, 12, early_fields, 0)

    for c in (*xheat, *yheat):
        c.wait_recv()
    for c in xyheat:
        c.wait_recv()
    unpack_x(HEAT)
    lane16, slot16, row8 = iota((16, 128), 1), iota((16, 128), 1) >> 3, iota((8, 128), 0)
    theirs = ((lane16 & 7) < 4, (lane16 & 7) >= 4)
    for p in range(2):
        ext[HEAT, LOW + p, inner] = jnp.where(theirs[p], hy[p], strips)
        ext[HEAT, LOW + p, outer] = jnp.where(row8 < 4, hxy[2 * p + 1], hxy[2 * p])
    mirror((HEAT, HEAT + 1), slice(0, 24))
    for d in range(2):
        new = (11, 2)[d]

        @pl.when(has[1 - d])
        def _(d=d, new=new):
            zheat[d].wait_recv()
            for k in (2 * d, 2 * d + 1):
                xzheat[k].wait_recv()
                yzheat[k].wait_recv()
            ext[HEAT, new, outer] = jnp.where(row8 < 4, hxz[2 * d + 1], hxz[2 * d])
            for p in range(2):
                ext[HEAT, LOW + p, inner] = jnp.where(
                    theirs[p] & (slot16 == new), pltpu.roll(hyz[2 * d + p], 64, 1), ext[HEAT, LOW + p, inner]
                )

        @pl.when(jnp.logical_not(has[1 - d]))
        def _(d=d, new=new):
            for p in range(2):
                v = ext[HEAT, LOW + p, inner]
                ext[HEAT, LOW + p, inner] = jnp.where(
                    theirs[p] & (slot16 == new), pltpu.roll(v, (8, 120)[d], 1), v
                )

    for c in youter:
        c.wait_recv()
    unpack_y(outer, 8)

    def step(src, dst, first, last):
        def drive(r, _):
            drives[r] = 6.0 * (1.0 - ext[HEAT, r, 0:24] - 0.5 * src[SOL, r, 0:24])
            return 0

        def sums(r, _):
            sums_of(src, r)
            return drive(r, 0)
        if first == 1:
            lax.fori_loop(1, 13, drive, 0, unroll=4)
        else:
            lax.fori_loop(first - 1, last + 1, sums, 0, unroll=(last + 2 - first) // 2)
        for r in (LOW, HIGH):
            sums(r, 0)
        final = dst is None
        groups = [(a, b, range(first, last)) for a, b in GROUPS[0:2]]
        if not final:
            groups.append((*GROUPS[2], range(first + 1, last - 1)))
        strips = groups[0 : 3 if first == 1 else 2]

        def fields(f, _):
            now = src.at[f]
            for a, b, rows in groups:
                edge = edges(now[LOW, a:b, :], now[HIGH, a:b, :])
                for r in rows:
                    if first == 1 and a and 3 <= r < 11:
                        continue
                    c, around = main_neighbours(now, r, a, edge)
                    v = grown(c, around, squares[r, a:b], drives[r, a:b])
                    if final:
                        grains_out[f, r - 3, a - 8 : b - 8, :] = v
                    else:
                        dst[f, r, a:b, :] = v
            if not final:
                for a, b, _ in strips:
                    for r in (LOW, HIGH):
                        c, around = strip_neighbours(now, r, a)
                        dst[f, r, a:b, :] = grown(c, around, squares[r, a:b], drives[r, a:b])
            return 0
        lax.fori_loop(0, 12, fields, 0)
        for a, b, rows in groups:
            edge = edges(bend[LOW, a:b, :], bend[HIGH, a:b, :])
            for r in rows:
                c, around = main_neighbours(bend, r, a, edge)
                v = src[SOL, r, a:b, :] + 0.15 * (around - 6.0 * c)
                if final:
                    solute_out[r - 3, a - 8 : b - 8, :] = v
                else:
                    dst[SOL, r, a:b, :] = v
        if not final:
            for a, b, _ in strips:
                for r in (LOW, HIGH):
                    c, around = strip_neighbours(bend, r, a)
                    dst[SOL, r, a:b, :] = src[SOL, r, a:b, :] + 0.15 * (around - 6.0 * c)

    step(ext, alt, 1, 13)
    for d in range(2):
        @pl.when(has[d])
        def _(d=d):
            for c in zcopy[d]:
                c.wait_send()

    step(alt, ext, 2, 12)
    step(ext, None, 3, 11)

    for c in [*request, *xcopy, *answer, *xheat, *yinner, *youter, *yheat, *xyheat]:
        c.wait_send()
    for d in range(2):
        @pl.when(has[d])
        def _(d=d):
            for k in (2 * d, 2 * d + 1):
                for c in (dcopy[k], xzheat[k], yzheat[k]):
                    c.wait_send()
            zheat[d].wait_send()
    if relays:
        @pl.when(relaying[0] | relaying[1])
        def _():
            onward[0].wait_send()


def body(grains, solute, thermal, block_slot, block_owner, block_offset):
    tiles = lax.axis_size("gz")
    vmem = pl.BlockSpec(memory_space=pltpu.VMEM)
    dma = pltpu.SemaphoreType.DMA
    import functools

    return pl.pallas_call(
        functools.partial(kernel, tiles),
        out_shape=(
            jax.ShapeDtypeStruct(grains.shape, F32),
            jax.ShapeDtypeStruct(solute.shape, F32),
            jax.ShapeDtypeStruct(solute.shape, F32),
        ),
        in_specs=[pl.BlockSpec(memory_space=pltpu.HBM)] * 6,
        out_specs=(vmem,) * 3,
        scratch_shapes=[
            pltpu.VMEM((NF, 16, 32, 128), F32),
            pltpu.VMEM((13, 16, 32, 128), F32),
            pltpu.VMEM((16, 32, 128), F32),
            pltpu.VMEM((16, 24, 128), F32),
            pltpu.VMEM((16, 24, 128), F32),
            pltpu.VMEM((2, NF, 24, 128), F32),
            pltpu.VMEM((2, NF, 24, 128), F32),
            pltpu.VMEM((13 - DIRECT, 24, 128), F32),
            pltpu.VMEM((4, 3, 16, 128), F32),
            pltpu.VMEM((4, 3, 16, 128), F32),
            pltpu.VMEM((13, 24, 128), F32),
            pltpu.VMEM((2, 13, 24, 128), F32),
            pltpu.VMEM((16, 128), F32),
            pltpu.VMEM((2, 16, 128), F32),
            pltpu.VMEM((4, 8, 128), F32),
            pltpu.VMEM((4, 8, 128), F32),
            pltpu.VMEM((4, 16, 128), F32),
            pltpu.VMEM((40, 4096), F32),
            pltpu.VMEM((5, 1, 20), jnp.int32),
            pltpu.VMEM((8, 128), F32),
            pltpu.VMEM((tiles, 8, 128), F32),
            pltpu.VMEM((5, 16, 16, 128), F32),
            pltpu.VMEM((7, 8, 128), F32),
            pltpu.VMEM((NODES, 640), F32),
            pltpu.VMEM((tiles, 24, 128), F32),
            pltpu.VMEM((tiles, 24, 128), F32),
            dma((6,)), dma((tiles,)), dma((tiles,)), dma((tiles,)), dma((tiles,)),
            dma((4,)), dma((4,)), dma((4,)), dma((4,)),
            dma((2,)), dma((2,)), dma((2,)), dma((2,)),
            dma((4,)), dma((4,)), dma((4,)), dma((4,)),
            dma, dma, dma((2,)), dma((2,)), dma((4,)), dma((4,)),
            dma((4,)), dma((4,)), dma((4,)), dma((4,)),
        ],
        compiler_params=pltpu.CompilerParams(
            collective_id=0, has_side_effects=True, vmem_limit_bytes=50331648
        ),
    )(*(
        pltpu.with_memory_space_constraint(a, pltpu.HBM)
        for a in (
            grains,
            solute,
            thermal.reshape(thermal.shape[3], thermal.shape[4]),
            block_slot.reshape(1, -1),
            block_owner.reshape(1, -1),
            block_offset.reshape(3, 1, -1),
        )
    ))


def solution(mesh):
    in_specs = (
        P(None, "gz", "gx", "gy"),
        P("gz", "gx", "gy"),
        P("gz", "gx", "gy", None, None),
        P("gz", "gx", "gy", None),
        P("gz", "gx", "gy", None),
        P("gz", "gx", "gy", None, None),
    )
    out_specs = (P(None, "gz", "gx", "gy"), P("gz", "gx", "gy"), P("gz", "gx", "gy"))
    return jax.shard_map(body, mesh=mesh, in_specs=in_specs, out_specs=out_specs, check_vma=False)
```

```python
import jax
import jax.numpy as jnp
from jax import lax
from jax.experimental import pallas as pl
from jax.experimental.pallas import tpu as pltpu
from jax.sharding import PartitionSpec as P

F32 = jnp.float32
BF16 = jnp.bfloat16
MESH = pl.DeviceIdType.MESH
NF = 14
SOL = 12
HEAT = 13
DIRECT = 5
EARLY = 7
KEY, HZ, HX, HY, LIVE, TILE = range(6)
AX = 9
NODES = 48
LOW, HIGH = 14, 15


def iota(shape, axis):
    return lax.broadcasted_iota(jnp.int32, shape, axis)


def split(x):
    high = x.astype(BF16)
    return high, (x - high.astype(F32)).astype(BF16)


def nt(a, b):
    return lax.dot_general(a, b, (((1,), (1,)), ((), ())), preferred_element_type=F32)


GROUPS = ((8, 16), (16, 24), (0, 8))


def edges(low, high):
    return jnp.where((iota(low.shape, 1) & 7) == 3, low, pltpu.roll(high, 126, 1))


def along_x(ref, r, a):
    sub = iota((8, 128), 0)
    if a == 0:
        before = jnp.where(sub == 0, ref[r, 23:24, :], pltpu.roll(ref[r, 0:8, :], 1, 0))
        return before + ref[r, 1:9, :]
    after = ref[r, a + 1 : a + 9, :]
    if a == 16:
        after = jnp.where(sub == 7, ref[r, 0:1, :], after)
    return ref[r, a - 1 : a + 7, :] + after


def main_neighbours(ref, r, a, edge):
    lane = iota((8, 128), 1)
    c = ref[r, a : a + 8, :]
    beyond = pltpu.roll(edge, (125 - r * 8) % 128, 1)
    left = jnp.where(lane == 0, beyond, pltpu.roll(c, 1, 1))
    right = jnp.where(lane == 127, beyond, pltpu.roll(c, 127, 1))
    return c, (ref[r - 1, a : a + 8, :] + ref[r + 1, a : a + 8, :]) + along_x(ref, r, a) + (left + right)


def strip_neighbours(ref, r, a):
    c = ref[r, a : a + 8, :]
    z = pltpu.roll(c, 8, 1) + pltpu.roll(c, 120, 1)
    y = pltpu.roll(c, 1, 1) + pltpu.roll(c, 127, 1)
    return c, z + y + along_x(ref, r, a)


def grown(c, around, s, drive):
    cc = c * c
    w = c - cc
    return w * ((0.4 * c - 0.2) + w * drive) + c * (0.1 * cc - s) + 0.16 * around


def kernel(
    tiles,
    grains, solute, thermal, slots, owners, offsets,
    grains_out, solute_out, heat_out,
    ext, alt, bend, squares, drives,
    xp, xr, relay, dp, dr, pk, yr,
    hk, hy, hxz, hxy, hyz,
    stored, lists_in, req, rq, lb, prm, xs, gr, gx,
    loads, s_rq, r_rq, s_gx, r_gx, s_z, r_z, s_x, r_x, s_zt, r_zt, s_xt, r_xt, s_d, r_d, s_y, r_y,
    s_relay, r_relay, s_hy, r_hy, s_hxz, r_hxz, s_hxy, r_hxy, s_hyz, r_hyz,
):
    me = lax.axis_index("gz")
    ix, iy = lax.axis_index("gx"), lax.axis_index("gy")
    nx, ny = lax.axis_size("gx"), lax.axis_size("gy")
    xside = ({"gx": lax.rem(ix + nx - 1, nx)}, {"gx": lax.rem(ix + 1, nx)})
    yside = ({"gy": lax.rem(iy + ny - 1, ny)}, {"gy": lax.rem(iy + 1, ny)})
    others = [{"gz": lax.rem(me + k, tiles)} for k in range(1, tiles)]
    has_low, has_high = me > 0, me < tiles - 1
    relays = nx == 8
    ax4 = lax.rem(ix, 4)
    far = (ax4 == 0, ax4 == 3) if relays else (ix < 0, ix < 0)
    relaying = (ax4 == 1, ax4 == 2)
    across = 6 + 2 * lax.rem(ix, 2) - ix
    zside = ({"gz": jnp.maximum(me - 1, 0)}, {"gz": jnp.minimum(me + 1, tiles - 1)})
    has = (has_low, has_high)

    bring = [
        pltpu.make_async_copy(slots, lists_in.at[0], loads.at[0]),
        pltpu.make_async_copy(owners, lists_in.at[1], loads.at[1]),
        pltpu.make_async_copy(offsets, lists_in.at[2:5], loads.at[2]),
        pltpu.make_async_copy(grains, ext.at[0:12, 3:11, 8:24], loads.at[3]),
        pltpu.make_async_copy(solute, ext.at[SOL, 3:11, 8:24], loads.at[4]),
        pltpu.make_async_copy(thermal, stored, loads.at[5]),
    ]
    for c in bring:
        c.start()

    barrier = pltpu.get_barrier_semaphore()
    xy = [[{**xside[s], **yside[t]} for s in range(2)] for t in range(2)]
    xz = [[{**xside[s], **zside[d]} for s in range(2)] for d in range(2)]
    yz = [[{**yside[t], **zside[d]} for d in range(2)] for t in range(2)]
    partners = [*xside, *yside, *others, *xy[0], *xy[1]]
    if relays:
        partners.append({"gx": across})
    for d in partners:
        pl.semaphore_signal(barrier, inc=1, device_id=d, device_id_type=MESH)
    for d in range(2):
        @pl.when(has[d])
        def _(d=d):
            for p in (*xz[d], yz[0][d], yz[1][d]):
                pl.semaphore_signal(barrier, inc=1, device_id=p, device_id_type=MESH)

    def remote(src, dst, ss, rs, d):
        return pltpu.make_async_remote_copy(
            src_ref=src, dst_ref=dst, send_sem=ss, recv_sem=rs, device_id=d, device_id_type=MESH
        )

    for c in bring[0:3]:
        c.wait()
    live = lists_in[1] >= 0
    livef = live.astype(F32)
    off = [lists_in[2 + i] for i in range(3)]
    req[...] = jnp.zeros((8, 128), F32)
    req[KEY : KEY + 1, 0:20] = jnp.where(live, lists_in[1] * 64 + lists_in[0], -1).astype(F32)
    for i in range(3):
        req[HZ + i : HZ + i + 1, 0:20] = ((off[i] + (off[i] & 1)) >> 1).astype(F32) * livef
    req[LIVE : LIVE + 1, 0:20] = livef
    req[TILE : TILE + 1, 0:20] = livef * me.astype(F32)

    for c in bring[3:5]:
        c.wait()
    for s, first in ((0, 0), (1, 13)):
        def pack(f, _, s=s, first=first):
            for i in range(3):
                xp[s, f, i * 8 : i * 8 + 8, :] = ext[f, 3:11, 8 + first + i, :]
            return 0
        lax.fori_loop(0, 13, pack, 0)

    pl.semaphore_wait(barrier, len(partners) + 4 * (jnp.minimum(me, 1) + jnp.minimum(tiles - 1 - me, 1)))

    request = [
        remote(req, rq.at[me], s_rq.at[k], r_rq.at[me], d) for k, d in enumerate(others)
    ]
    for c in request:
        c.start()
    xcopy = []
    for s in range(2):
        xcopy.append(remote(xp.at[s, 0:DIRECT], xr.at[1 - s, 0:DIRECT], s_x.at[s], r_x.at[1 - s], xside[s]))
    for s in range(2):
        xcopy.append(remote(
            xp.at[s, DIRECT:13], xr.at[1 - s, DIRECT:13], s_x.at[2 + s], r_x.at[3 - s], xside[s]
        ))
    by_way = [remote(xp.at[s, DIRECT:13], relay, s_x.at[2 + s], r_relay, xside[1 - s]) for s in range(2)]
    onward = [
        remote(relay, xr.at[1 - s, DIRECT:13], s_relay, r_x.at[3 - s], {"gx": across}) for s in range(2)
    ]
    if relays:
        for s in range(2):
            @pl.when(far[s])
            def _(s=s):
                by_way[s].start()
    for s in range(2):
        xcopy[s].start()
    for s in range(2):
        @pl.when(jnp.logical_not(far[s]))
        def _(s=s):
            xcopy[2 + s].start()
    zrows = ((0, 11), (5, 0))
    zcopy = []
    for d in range(2):
        a, b = zrows[d]
        zcopy.append([
            remote(
                ext.at[f, 3 + a : 6 + a, 8:24], ext.at[f, b : b + 3, 8:24], s_z.at[2 * k + d], r_z.at[2 * k + d], zside[d]
            )
            for k, f in enumerate((slice(0, EARLY), slice(EARLY, 13)))
        ])

        @pl.when(has[d])
        def _(d=d):
            zcopy[d][0].start()


    row8, lane8 = iota((8, 128), 0), iota((8, 128), 1) >> 4
    bring[5].wait()

    def turn(g, _):
        rows = pl.ds(pl.multiple_of(g * 8, 8), 8)
        for c in range(32):
            v = stored[rows, c * 128 : c * 128 + 128]
            for k in (1, 2, 4):
                rb, lbit = (row8 & k) != 0, (lane8 & k) != 0
                a = pltpu.roll(pltpu.roll(v, 8 - k, 0), 16 * k, 1)
                b = pltpu.roll(pltpu.roll(v, k, 0), 128 - 16 * k, 1)
                v = jnp.where(rb == lbit, v, jnp.where(lbit, a, b))
            lb[g, c // 2, (c % 2) * 8 : (c % 2) * 8 + 8, :] = v
        return 0
    lax.fori_loop(0, 5, turn, 0)
    rq[me] = req[...]
    xs[...] = jnp.zeros(xs.shape, F32)

    for k in range(1, tiles):
        src = lax.rem(me + tiles - k, tiles)
        remote(req, rq.at[src], s_rq.at[k - 1], r_rq.at[src], others[k - 1]).wait_recv()

    if relays:
        for s in range(2):
            @pl.when(relaying[s])
            def _(s=s):
                by_way[s].wait_recv()
                onward[s].start()

    lists = [jnp.zeros((8, 128), F32), jnp.zeros((8, 128), F32)]
    for t in range(tiles):
        v = rq[t]
        lists[t // 4] = lists[t // 4] + (pltpu.roll(v, 32 * (t % 4), 1) if t % 4 else v)
    for h in range(2):
        prm[5 + h] = lists[h]
    base = me * 64
    for g in range(5):
        slot_of = base + g * 8 + (iota((128, 128), 0) >> 4)
        total = jnp.zeros((8, 128), F32)
        for h in range(2):
            match = jnp.where(lists[h][KEY : KEY + 1, :] == slot_of.astype(F32), 1.0, 0.0).astype(BF16)
            total = total + nt(lists[h].astype(BF16), match)
        prm[g] = total

    def choose(g, _):
        v = prm[g]
        hz, hx = v[HZ : HZ + 1, :], v[HX : HX + 1, :]
        layers = [jnp.zeros((16, 128), F32) for _ in range(5)]
        for p in range(16):
            part = lb[g, p]
            for a in range(5):
                layers[a] = layers[a] + jnp.where(hz == float(a - p), part, 0.0)
        at = iota((16, 128), 0).astype(F32) + hx
        lanes = pl.ds(pl.multiple_of(g * 128, 128), 128)
        for a in range(5):
            for b in range(AX):
                xs[a * AX + b : a * AX + b + 1, lanes] = jnp.sum(
                    jnp.where(at == float(b), layers[a], 0.0), axis=0, keepdims=True
                )
        return 0
    lax.fori_loop(0, 5, choose, 0)

    hi, lo = split(xs[...])
    both = jnp.concatenate([hi, lo], axis=0)
    where_to = []
    for g in range(5):
        v = prm[g]
        spot = v[HY : HY + 1, :] + 128.0 * v[TILE : TILE + 1, :] + (iota((1, 128), 1) & 15).astype(F32)
        where_to.append(jnp.where(v[LIVE : LIVE + 1, :] > 0.5, spot, -4096.0))
    where_to = jnp.concatenate(where_to, axis=1)
    tile_of = lax.rem(me + iota((8, 640), 0), tiles) * 128 + 64
    last = jnp.where(tile_of.astype(F32) == where_to, 1.0, 0.0).astype(BF16)
    blank = jnp.zeros((64, 640), BF16)
    tail = nt(last, jnp.concatenate([blank, hi, blank[0:16]], axis=0))
    tail = tail + nt(last, jnp.concatenate([blank, lo, blank[0:16]], axis=0))
    lane, at_last = iota((24, 128), 1), iota((24, 128), 0) == 23
    answer = []
    for k in range(tiles - 1, -1, -1):
        t = lax.rem(me + k, tiles)
        line = (iota((128, 640), 0) + t * 128).astype(F32)
        onto = jnp.where(line == where_to, 1.0, 0.0).astype(BF16)
        out = nt(both, onto)
        out = out[0:NODES] + out[NODES : 2 * NODES]
        upper = jnp.where(at_last, tail[k : k + 1, :], pltpu.roll(out[24:48], 64, 1))
        gr[t] = jnp.where(lane < 64, out[0:24], upper)
        if k:
            c = remote(gr.at[t], gx.at[me], s_gx.at[k - 1], r_gx.at[me], others[k - 1])
            c.start()
            answer.append(c)

    for d in range(2):
        @pl.when(has[d])
        def _(d=d):
            zcopy[d][1].start()

    inner, outer = slice(8, 24), slice(0, 8)
    def mirror(fields, rows):
        for d in range(2):
            @pl.when(jnp.logical_not(has[1 - d]))
            def _(d=d):
                def one(f, _):
                    for i in range(3):
                        if d:
                            ext[f, 2 - i, rows] = ext[f, 3 + i, rows]
                        else:
                            ext[f, 11 + i, rows] = ext[f, 10 - i, rows]
                    return 0
                lax.fori_loop(*fields, one, 0)

    def pack_y(rows, count):
        slot = iota((count, 128), 1) >> 3
        def one(f, _):
            v = jnp.zeros((count, 128), F32)
            for r in range(14):
                v = jnp.where(slot == r, pltpu.roll(ext[f, r, rows], r * 8 + 4, 1), v)
            pk[f, rows] = v
            return 0
        lax.fori_loop(0, 13, one, 0)

    def y_copies(rows, k):
        return [
            remote(pk.at[:, rows], yr.at[1, :, rows], s_y.at[k], r_y.at[k + 1], yside[0]),
            remote(pk.at[:, rows], yr.at[0, :, rows], s_y.at[k + 1], r_y.at[k], yside[1]),
        ]

    def unpack_y(rows, count):
        upper = (iota((count, 128), 1) & 7) >= 4
        def one(f, _):
            own = pk[f, rows]
            ext[f, LOW, rows] = jnp.where(upper, own, yr[0, f, rows])
            ext[f, HIGH, rows] = jnp.where(upper, yr[1, f, rows], own)
            return 0
        lax.fori_loop(0, 13, one, 0)

    def unpack_x(f):
        for z in range(8):
            ext[f, 3 + z, 0:3, :] = xr[1, f, pl.ds(z, 3, stride=8), :]
            ext[f, 3 + z, 5:8, :] = xr[0, f, pl.ds(z, 3, stride=8), :]

    bz, bx, by = [
        jnp.max(jnp.where(live, o & 1, 0).astype(F32), axis=1, keepdims=True) for o in off
    ]
    node, cell = iota((128, 128), 0), iota((128, 128), 1).astype(F32)
    wy = jnp.maximum(0.0, 1.0 - jnp.abs(cell - (2.0 * node.astype(F32) - by)) * 0.5)
    wy = jnp.where(node < 64, wy, 0.0).astype(BF16)
    w64 = jnp.maximum(0.0, 1.0 - jnp.abs(iota((1, 128), 1).astype(F32) - (128.0 - by)) * 0.5)
    ci, ki = iota((128, NODES), 0), iota((128, NODES), 1)
    az = (ki * 57) >> 9
    ax = ki - AX * az
    wz = jnp.maximum(0.0, 1.0 - jnp.abs((ci >> 4).astype(F32) - (2.0 * az.astype(F32) - bz)) * 0.5)
    wx = jnp.maximum(0.0, 1.0 - jnp.abs((ci & 15).astype(F32) - (2.0 * ax.astype(F32) - bx)) * 0.5)
    wzx32 = wz * wx
    wzx = wzx32.astype(BF16)

    grid = gr[me]
    for k in range(1, tiles):
        src = lax.rem(me + tiles - k, tiles)
        remote(gr.at[src], gx.at[src], s_gx.at[k - 1], r_gx.at[src], others[k - 1]).wait_recv()
        grid = grid + gx[src]
    turned = pltpu.roll(grid, 64, 1)
    column = jnp.sum(wzx32 * turned[23:24, 0:NODES], axis=1, keepdims=True)
    hi, lo = split(jnp.concatenate([grid, turned], axis=0))
    fine = jnp.dot(jnp.concatenate([hi, lo], axis=0), wy, preferred_element_type=F32)
    fine = fine[0:NODES] + fine[NODES : 2 * NODES]
    hi, lo = split(fine)
    heat = jnp.dot(wzx, hi, preferred_element_type=F32) + jnp.dot(wzx, lo, preferred_element_type=F32)
    heat = heat + column * w64
    heat = heat.reshape(8, 16, 128)
    heat_out[...] = heat
    for z in range(8):
        ext[HEAT, 3 + z, 8:24, :] = heat[z]
    for s, first in ((0, 0), (1, 13)):
        for i in range(3):
            xp[s, HEAT, i * 8 : i * 8 + 8, :] = heat[:, first + i, :]
    xheat = [
        remote(xp.at[0, HEAT], xr.at[1, HEAT], s_xt.at[0], r_xt.at[1], xside[0]),
        remote(xp.at[1, HEAT], xr.at[0, HEAT], s_xt.at[1], r_xt.at[0], xside[1]),
    ]
    for c in xheat:
        c.start()
    zheat = []
    for d in range(2):
        a, b = zrows[d]
        zheat.append(remote(
            ext.at[HEAT, 3 + a : 6 + a, 8:24], ext.at[HEAT, b : b + 3, 8:24], s_zt.at[d], r_zt.at[d], zside[d]
        ))

        @pl.when(has[d])
        def _(d=d):
            zheat[d].start()

    for z in range(8):
        v = pltpu.roll(heat[z], (z + 3) * 8 + 4, 1)
        strips = v if z == 0 else jnp.where((iota((16, 128), 1) >> 3) == z + 3, v, strips)
    hk[...] = strips
    yheat, xyheat, xzheat, yzheat = [], [], [], []
    for t in range(2):
        yheat.append(remote(hk, hy.at[1 - t], s_hy.at[t], r_hy.at[1 - t], yside[t]))
        for s in range(2):
            n = 2 * (1 - t) + 1 - s
            xyheat.append(remote(
                hk.at[8 * s : 8 * s + 8], hxy.at[n], s_hxy.at[2 * t + s], r_hxy.at[n], xy[t][s]
            ))
    for c in (*xyheat, *yheat):
        c.start()
    for d in range(2):
        for s in range(2):
            n = 2 * d + 1 - s
            xzheat.append(remote(
                ext.at[HEAT, (3, 10)[d], 8 * s + 8 : 8 * s + 16], hxz.at[n], s_hxz.at[2 * d + s], r_hxz.at[n], xz[d][s]
            ))
        for t in range(2):
            n = 2 * d + 1 - t
            yzheat.append(remote(hk, hyz.at[n], s_hyz.at[2 * d + t], r_hyz.at[n], yz[t][d]))

        @pl.when(has[d])
        def _(d=d):
            for k in (2 * d, 2 * d + 1):
                xzheat[k].start()
                yzheat[k].start()

    for c in xcopy:
        c.wait_recv()

    order = ((2, 1), (0, 1))
    shown = ((0, 1), (7, 6))
    dcopy = []
    for d in range(2):
        for s in range(2):
            near, far = order[s]
            z1, z2 = shown[d]
            for k, (i, z) in enumerate(((near, z1), (near, z2), (far, z1))):
                for f in range(13):
                    dp[2 * d + s, k, f : f + 1, :] = xr[s, f, i * 8 + z : i * 8 + z + 1, :]
            dcopy.append(remote(
                dp.at[2 * d + s], dr.at[2 * d + s], s_d.at[2 * d + s], r_d.at[2 * d + s], zside[d]
            ))

        @pl.when(has[d])
        def _(d=d):
            for s in range(2):
                dcopy[2 * d + s].start()

    def unpack_all(f, _):
        unpack_x(f)
        return 0
    lax.fori_loop(0, 13, unpack_all, 0)

    for d in range(2):
        @pl.when(has[1 - d])
        def _(d=d):
            for c in zcopy[d]:
                c.wait_recv()
    mirror((0, 13), inner)
    pack_y(inner, 16)
    yinner = y_copies(inner, 0)
    for c in yinner:
        c.start()

    for d in range(2):
        @pl.when(has[1 - d])
        def _(d=d):
            for s in range(2):
                dcopy[2 * d + s].wait_recv()
            e1, e2 = ((11, 12), (2, 1))[d]
            for s in range(2):
                x1, x2 = ((7, 6), (0, 1))[s]
                for k, (e, x) in enumerate(((e1, x1), (e2, x1), (e1, x2))):
                    for f in range(13):
                        ext[f, e, x : x + 1, :] = dr[2 * d + s, k, f : f + 1, :]
    mirror((0, 13), outer)

    pack_y(outer, 8)
    youter = y_copies(outer, 2)
    for c in youter:
        c.start()

    for c in yinner:
        c.wait_recv()
    unpack_y(inner, 16)

    def sums_of(src, r):
        cells = slice(0, 24)
        s = src[0, r, cells] * src[0, r, cells]
        for f in range(1, 12):
            s = s + src[f, r, cells] * src[f, r, cells]
        squares[r] = 0.1 * s - 0.04
        bend[r, cells] = src[SOL, r, cells] - 0.5 * s

    def early_sums(r, _):
        sums_of(ext, r)
        return 0
    lax.fori_loop(0, 14, early_sums, 0, unroll=2)
    for r in range(3, 11):
        drives[r, inner] = 6.0 * (1.0 - ext[HEAT, r, inner] - 0.5 * ext[SOL, r, inner])

    def early_fields(f, _):
        now = ext.at[f]
        for a, b in GROUPS[0:2]:
            edge = edges(now[LOW, a:b, :], now[HIGH, a:b, :])
            for r in range(3, 11):
                c, around = main_neighbours(now, r, a, edge)
                alt[f, r, a:b, :] = grown(c, around, squares[r, a:b], drives[r, a:b])
        return 0
    lax.fori_loop(0, 12, early_fields, 0)

    for c in (*xheat, *yheat):
        c.wait_recv()
    for c in xyheat:
        c.wait_recv()
    unpack_x(HEAT)
    lane16, slot16, row8 = iota((16, 128), 1), iota((16, 128), 1) >> 3, iota((8, 128), 0)
    theirs = ((lane16 & 7) < 4, (lane16 & 7) >= 4)
    for p in range(2):
        ext[HEAT, LOW + p, inner] = jnp.where(theirs[p], hy[p], strips)
        ext[HEAT, LOW + p, outer] = jnp.where(row8 < 4, hxy[2 * p + 1], hxy[2 * p])
    mirror((HEAT, HEAT + 1), slice(0, 24))
    for d in range(2):
        new = (11, 2)[d]

        @pl.when(has[1 - d])
        def _(d=d, new=new):
            zheat[d].wait_recv()
            for k in (2 * d, 2 * d + 1):
                xzheat[k].wait_recv()
                yzheat[k].wait_recv()
            ext[HEAT, new, outer] = jnp.where(row8 < 4, hxz[2 * d + 1], hxz[2 * d])
            for p in range(2):
                ext[HEAT, LOW + p, inner] = jnp.where(
                    theirs[p] & (slot16 == new), pltpu.roll(hyz[2 * d + p], 64, 1), ext[HEAT, LOW + p, inner]
                )

        @pl.when(jnp.logical_not(has[1 - d]))
        def _(d=d, new=new):
            for p in range(2):
                v = ext[HEAT, LOW + p, inner]
                ext[HEAT, LOW + p, inner] = jnp.where(
                    theirs[p] & (slot16 == new), pltpu.roll(v, (8, 120)[d], 1), v
                )

    for c in youter:
        c.wait_recv()
    unpack_y(outer, 8)

    def step(src, dst, first, last):
        def drive(r, _):
            drives[r] = 6.0 * (1.0 - ext[HEAT, r, 0:24] - 0.5 * src[SOL, r, 0:24])
            return 0

        def sums(r, _):
            sums_of(src, r)
            return drive(r, 0)
        if first == 1:
            lax.fori_loop(1, 13, drive, 0, unroll=4)
        else:
            lax.fori_loop(first - 1, last + 1, sums, 0, unroll=(last + 2 - first) // 2)
        for r in (LOW, HIGH):
            sums(r, 0)
        final = dst is None
        groups = [(a, b, range(first, last)) for a, b in GROUPS[0:2]]
        if not final:
            groups.append((*GROUPS[2], range(first + 1, last - 1)))
        strips = groups[0 : 3 if first == 1 else 2]

        def fields(f, _):
            now = src.at[f]
            for a, b, rows in groups:
                edge = edges(now[LOW, a:b, :], now[HIGH, a:b, :])
                for r in rows:
                    if first == 1 and a and 3 <= r < 11:
                        continue
                    c, around = main_neighbours(now, r, a, edge)
                    v = grown(c, around, squares[r, a:b], drives[r, a:b])
                    if final:
                        grains_out[f, r - 3, a - 8 : b - 8, :] = v
                    else:
                        dst[f, r, a:b, :] = v
            if not final:
                for a, b, _ in strips:
                    for r in (LOW, HIGH):
                        c, around = strip_neighbours(now, r, a)
                        dst[f, r, a:b, :] = grown(c, around, squares[r, a:b], drives[r, a:b])
            return 0
        lax.fori_loop(0, 12, fields, 0)
        for a, b, rows in groups:
            edge = edges(bend[LOW, a:b, :], bend[HIGH, a:b, :])
            for r in rows:
                c, around = main_neighbours(bend, r, a, edge)
                v = src[SOL, r, a:b, :] + 0.15 * (around - 6.0 * c)
                if final:
                    solute_out[r - 3, a - 8 : b - 8, :] = v
                else:
                    dst[SOL, r, a:b, :] = v
        if not final:
            for a, b, _ in strips:
                for r in (LOW, HIGH):
                    c, around = strip_neighbours(bend, r, a)
                    dst[SOL, r, a:b, :] = src[SOL, r, a:b, :] + 0.15 * (around - 6.0 * c)

    step(ext, alt, 1, 13)
    for d in range(2):
        @pl.when(has[d])
        def _(d=d):
            for c in zcopy[d]:
                c.wait_send()

    step(alt, ext, 2, 12)
    step(ext, None, 3, 11)

    for c in [*request, *xcopy, *answer, *xheat, *yinner, *youter, *yheat, *xyheat]:
        c.wait_send()
    for d in range(2):
        @pl.when(has[d])
        def _(d=d):
            for k in (2 * d, 2 * d + 1):
                for c in (dcopy[k], xzheat[k], yzheat[k]):
                    c.wait_send()
            zheat[d].wait_send()
    if relays:
        @pl.when(relaying[0] | relaying[1])
        def _():
            onward[0].wait_send()


def body(grains, solute, thermal, block_slot, block_owner, block_offset):
    tiles = lax.axis_size("gz")
    vmem = pl.BlockSpec(memory_space=pltpu.VMEM)
    dma = pltpu.SemaphoreType.DMA
    import functools

    return pl.pallas_call(
        functools.partial(kernel, tiles),
        out_shape=(
            jax.ShapeDtypeStruct(grains.shape, F32),
            jax.ShapeDtypeStruct(solute.shape, F32),
            jax.ShapeDtypeStruct(solute.shape, F32),
        ),
        in_specs=[pl.BlockSpec(memory_space=pltpu.HBM)] * 6,
        out_specs=(vmem,) * 3,
        scratch_shapes=[
            pltpu.VMEM((NF, 16, 32, 128), F32),
            pltpu.VMEM((13, 16, 32, 128), F32),
            pltpu.VMEM((16, 32, 128), F32),
            pltpu.VMEM((16, 24, 128), F32),
            pltpu.VMEM((16, 24, 128), F32),
            pltpu.VMEM((2, NF, 24, 128), F32),
            pltpu.VMEM((2, NF, 24, 128), F32),
            pltpu.VMEM((13 - DIRECT, 24, 128), F32),
            pltpu.VMEM((4, 3, 16, 128), F32),
            pltpu.VMEM((4, 3, 16, 128), F32),
            pltpu.VMEM((13, 24, 128), F32),
            pltpu.VMEM((2, 13, 24, 128), F32),
            pltpu.VMEM((16, 128), F32),
            pltpu.VMEM((2, 16, 128), F32),
            pltpu.VMEM((4, 8, 128), F32),
            pltpu.VMEM((4, 8, 128), F32),
            pltpu.VMEM((4, 16, 128), F32),
            pltpu.VMEM((40, 4096), F32),
            pltpu.VMEM((5, 1, 20), jnp.int32),
            pltpu.VMEM((8, 128), F32),
            pltpu.VMEM((tiles, 8, 128), F32),
            pltpu.VMEM((5, 16, 16, 128), F32),
            pltpu.VMEM((7, 8, 128), F32),
            pltpu.VMEM((NODES, 640), F32),
            pltpu.VMEM((tiles, 24, 128), F32),
            pltpu.VMEM((tiles, 24, 128), F32),
            dma((6,)), dma((tiles,)), dma((tiles,)), dma((tiles,)), dma((tiles,)),
            dma((4,)), dma((4,)), dma((4,)), dma((4,)),
            dma((2,)), dma((2,)), dma((2,)), dma((2,)),
            dma((4,)), dma((4,)), dma((4,)), dma((4,)),
            dma, dma, dma((2,)), dma((2,)), dma((4,)), dma((4,)),
            dma((4,)), dma((4,)), dma((4,)), dma((4,)),
        ],
        compiler_params=pltpu.CompilerParams(
            collective_id=0, has_side_effects=True, vmem_limit_bytes=50331648
        ),
    )(*(
        pltpu.with_memory_space_constraint(a, pltpu.HBM)
        for a in (
            grains,
            solute,
            thermal.reshape(thermal.shape[3], thermal.shape[4]),
            block_slot.reshape(1, -1),
            block_owner.reshape(1, -1),
            block_offset.reshape(3, 1, -1),
        )
    ))


def solution(mesh):
    in_specs = (
        P(None, "gz", "gx", "gy"),
        P("gz", "gx", "gy"),
        P("gz", "gx", "gy", None, None),
        P("gz", "gx", "gy", None),
        P("gz", "gx", "gy", None),
        P("gz", "gx", "gy", None, None),
    )
    out_specs = (P(None, "gz", "gx", "gy"), P("gz", "gx", "gy"), P("gz", "gx", "gy"))
    return jax.shard_map(body, mesh=mesh, in_specs=in_specs, out_specs=out_specs, check_vma=False)
```
